32 devices in a mesh: rng: 2 (over x), az: 16 (over z, y, core).
Axes of the slice: x: 2, y: 2, z: 4, core: 2. Of those that a mesh axis runs over, the one named last changes fastest.
Arguments:
- spectrum: float32 [1024, 2, 32768], P('rng', None, 'az'), may hold values from -9 to 9
- src_block: int32 [256, 8], P('az', 'rng'), may hold values from 0 to 6, as said below
- offsets: int32 [256, 1024], P('az', 'rng'), may hold values from 0 to 127
- tap_weights: float32 [8, 256, 1024], P(None, 'az', 'rng'), may hold values from -2 to 2
Outputs:
- image: float32 [1024, 2, 32768], P(('rng', 'az'))
The draws below stay inside these ranges and needn't reach their ends.
Inputs may be any that keep to these rules, and one draw needn't show every extreme that they name: src_block[g, b] lies between min(b, 6) and min(b + 5, 6); a shift of 5 blocks occurs in every draw.
All inputs are finite; a program needn't handle non-finite values.
Results may differ from the reference program's by a relative error of at most 0.00007.
Values sent between devices are 32-bit elements; how exact they have to be, the bound alone decides.
A program may use at most 192 MiB of HBM per device.

```python
import jax
import jax.numpy as jnp
from jax import lax

NA = 32768
NRB = 1024
BLOCK = 128
GW = 128
TAPS = 8
SHIFT_B = 5
NG = 256
NOB = 8


def draw_spectrum(key, part):
    position = jnp.arange(NRB, dtype=jnp.float32) / NRB
    noise = jnp.clip(jax.random.normal(key, (NRB, 2, NA), jnp.float32), -5.0, 5.0)
    amplitude = jnp.sqrt(1.0 + 2.0 * position)
    return noise * amplitude[:, None, None]


def draw_src_block(key, part):
    groups = jnp.arange(NG, dtype=jnp.int32)
    blocks = jnp.arange(NOB, dtype=jnp.int32)
    distance = jnp.abs(2 * groups + 1 - NG)
    baseline = SHIFT_B * distance // NG
    jitter = jax.random.randint(key, (NG, NOB), 0, 2).astype(jnp.int32)
    shifted = jnp.minimum(baseline[:, None] + jitter, SHIFT_B)
    shifted = jnp.where(groups[:, None] == 0, SHIFT_B, shifted)
    return jnp.minimum(blocks[None, :] + shifted, NOB - 2).astype(jnp.int32)


def place_ends(result, rng, smallest, largest):
    index_at = [jax.random.randint(jax.random.fold_in(rng, axis), (), 0, length) for axis, length in enumerate(result.shape)]
    widest = result.shape.index(max(result.shape))
    beside = index_at[:widest] + [(index_at[widest] + 1) % result.shape[widest]] + index_at[widest + 1:]
    return result.at[tuple(index_at)].set(smallest).at[tuple(beside)].set(largest)


def block_levels(key, shape, shards, smallest, high):
    loudness, own = 1.0, jax.random.fold_in(key, 6)
    for axis_at, parts in shards:
        heights = jnp.exp(jax.random.uniform(jax.random.fold_in(own, axis_at), (parts,), jnp.float32, smallest / len(shards), high / len(shards)))
        loudness = loudness * jnp.repeat(heights, shape[axis_at] // parts).reshape([-1 if axis == axis_at else 1 for axis in range(len(shape))])
    return loudness


def scatter_about(stream_key, dims, spread, reach, split=(), held_as=jnp.bfloat16):
    level = block_levels(stream_key, dims, split, -0.22, 0.18) if split else 1.0
    entries = jax.random.normal(stream_key, dims, jnp.float32) * spread * level
    return jnp.minimum(jnp.maximum(entries, -reach), reach).astype(held_as)


def setup_inputs(seed: int = 0) -> dict:
    keys = jax.random.split(jax.random.key(seed), 5)
    spectrum = draw_spectrum(jax.random.fold_in(keys[4], 71), 0)
    src_block = draw_src_block(jax.random.fold_in(keys[4], 71), 0)
    offsets = place_ends(jax.random.randint(keys[2], (NG, NRB), 0, BLOCK), jax.random.fold_in(keys[2], 1), 0, BLOCK - 1).astype(jnp.int32)
    tap_weights = scatter_about(keys[3], (TAPS, NG, NRB), 0.35, 2.0, ((1, 16), (2, 2)), jnp.float32)
    return dict(spectrum=spectrum, src_block=src_block, offsets=offsets, tap_weights=tap_weights)


def reference(spectrum, src_block, offsets, tap_weights):
    grouped = spectrum.reshape(NRB, 2, NG, GW).transpose(2, 0, 1, 3).reshape(NG, NRB, 2 * GW)
    src_rows = (src_block[:, :, None] * BLOCK + offsets.reshape(NG, NOB, BLOCK)).reshape(NG, NRB).astype(jnp.int32)

    def pick(table, where):
        return jnp.take(table, where, axis=0)
    remapped = jnp.zeros((NG, NRB, 2 * GW), jnp.float32)
    for tap_index in range(TAPS):
        picked = jax.vmap(pick)(grouped, src_rows + tap_index)
        remapped = remapped + tap_weights[tap_index][:, :, None] * picked
    remapped = remapped.reshape(NG, NRB, 2, GW).transpose(1, 2, 0, 3).reshape(NRB, 2, NA)
    values = jnp.fft.ifft(remapped[:, 0] + 1j * remapped[:, 1], axis=-1)
    band = jnp.stack([jnp.real(values), jnp.imag(values)], axis=1).astype(jnp.float32)
    energy = jnp.sum(band * band)
    scaling = lax.rsqrt(energy / (NRB * NA) + 1e-06)
    return band * scaling
```

```python
import functools

import jax
import jax.numpy as jnp
import numpy as np
from jax import lax
from jax.experimental import pallas as pl
from jax.experimental.pallas import tpu as pltpu
from jax.sharding import PartitionSpec as P

BLOCK = 128
GW = 128
TAPS = 8
SHIFT_B = 5
WINDOW = 144
LAG = 2
STEP = 4

MESH = pl.DeviceIdType.MESH


def split_np(x):
    hi = x.astype(jnp.bfloat16)
    lo = (x - hi.astype(np.float64)).astype(jnp.bfloat16)
    return hi, lo


def split(x):
    hi = x.astype(jnp.bfloat16)
    lo = (x - hi.astype(jnp.float32)).astype(jnp.bfloat16)
    return hi, lo


def plan(groups):
    last = max(1, groups // 4)
    single = min(groups - last, (3 * groups) // 8)
    sizes = [1] * single
    left = groups - last - single
    sizes += [2] * (left // 2) + [1] * (left % 2) + [last]
    starts = [sum(sizes[:i]) for i in range(len(sizes))]
    return tuple(zip(starts, sizes))


def dft_tables(az_count, groups, chunks):
    total_groups = az_count * groups
    total_len = total_groups * GW
    k1 = np.arange(total_groups)
    stage_one = []
    for start, per in chunks:
        gl, az = np.meshgrid(np.arange(start, start + per), np.arange(az_count), indexing="ij")
        g = az * groups + gl
        angle = 2.0 * np.pi * ((k1[:, None, None] * g[None]) % total_groups) / total_groups
        first = np.empty((2, total_groups, per, 2, az_count))
        first[0, :, :, 0] = np.cos(angle)
        first[0, :, :, 1] = -np.sin(angle)
        first[1, :, :, 0] = np.sin(angle)
        first[1, :, :, 1] = np.cos(angle)
        hi, lo = split_np(first.reshape(2 * total_groups, 2 * per * az_count))
        stage_one.append(np.concatenate([hi, hi, lo], axis=1))
    l = np.arange(GW)
    turn = 2.0 * np.pi * (k1[:, None] * l[None, :]) / total_len
    twist = np.stack([np.cos(turn), np.sin(turn)]).astype(np.float32) / np.float32(total_len)
    inner = 2.0 * np.pi * ((l[:, None] * l[None, :]) % GW) / GW
    second = np.empty((2, GW, 2, GW))
    second[0, :, 0] = np.cos(inner)
    second[0, :, 1] = -np.sin(inner)
    second[1, :, 0] = np.sin(inner)
    second[1, :, 1] = np.cos(inner)
    b_hi, b_lo = split_np(second.reshape(2 * GW, 2 * GW))
    return stage_one + [twist, b_hi, b_lo]


def remap_group(ext, out, sub, gl, blocks, src_of, off_row, weight_row):
    energy = jnp.zeros((8, GW), jnp.float32)
    for b in range(blocks):
        start = src_of(b) * (BLOCK * 2)
        source = jnp.concatenate(
            [ext[pl.ds(start + c, WINDOW, stride=2), :] for c in range(2)], axis=1
        )
        at = lax.broadcasted_iota(jnp.int32, (WINDOW, BLOCK), 0) - off_row(b)
        taps = jnp.zeros((WINDOW, BLOCK), jnp.float32)
        for t in range(TAPS):
            taps = jnp.where(at == t, weight_row(t, b), taps)
        t_hi, t_lo = split(taps)
        s_hi, s_lo = split(source)
        left = jnp.concatenate([t_hi, t_lo, t_hi], axis=0)
        right = jnp.concatenate([s_hi, s_hi, s_lo], axis=0)
        value = lax.dot_general(
            left, right, (((0,), (0,)), ((), ())), preferred_element_type=jnp.float32
        )
        for c in range(2):
            half = value[:, c * GW:(c + 1) * GW]
            out[pl.ds(b * BLOCK * sub + 2 * gl + c, BLOCK, stride=sub), :] = half
            energy = energy + jnp.sum((half * half).reshape(BLOCK // 8, 8, GW), axis=0)
    return energy


def fused_kernel(rows, blocks, groups, chunks, counts, step, cells, src_ref, off_hbm, w_hbm, spec_ref, *rest):
    n = len(chunks)
    tables_hbm, image_ref, scratch = rest[:n + 3], rest[n + 3], rest[n + 4:]
    ext, scratch = scratch[:groups], scratch[groups:]
    stage, scratch = scratch[:n], scratch[n:]
    recv, scratch = scratch[:n], scratch[n:]
    tables, scratch = scratch[:n + 3], scratch[n + 3:]
    (y_acc, off_ref, w_ref, e_own, e_az, e_sum, e_rng, small_sem, table_sem, local_sem, halo_send, halo_recv,
     part_send, part_recv, last_recv, e_send, e_recv) = scratch
    a_refs, (twist_ref, b_hi_ref, b_lo_ref) = tables[:n], tables[n:]
    rng_count, az_count = lax.axis_size("rng"), lax.axis_size("az")
    p, q = lax.axis_index("rng"), lax.axis_index("az")
    piece = rows // az_count
    half = max(az_count // 2, 1)
    side, place = q // half, q % half
    subsets = piece // step
    total_groups = az_count * groups
    wide = 2 * GW

    def local(g):
        return pltpu.make_async_copy(
            spec_ref.at[:, g], ext[g].at[pl.ds(0, rows)], local_sem.at[g])

    def halo(g, i):
        return pltpu.make_async_remote_copy(
            src_ref=spec_ref.at[pl.ds(0, counts[i]), g],
            dst_ref=ext[g].at[pl.ds(rows + sum(counts[:i]), counts[i])],
            send_sem=halo_send.at[g, i], recv_sem=halo_recv.at[g, i],
            device_id={"rng": (p + rng_count - i - 1) % rng_count}, device_id_type=MESH)

    def table(i):
        return pltpu.make_async_copy(tables_hbm[i], tables[i], table_sem.at[i])

    small = [pltpu.make_async_copy(off_hbm, off_ref, small_sem.at[0]),
             pltpu.make_async_copy(w_hbm, w_ref, small_sem.at[1])]
    for copy in small:
        copy.start()
    local(0).start()

    barrier = pltpu.get_barrier_semaphore()

    @pl.loop(1, rng_count)
    def _(j):
        pl.semaphore_signal(barrier, inc=1, device_id={"rng": (p + j) % rng_count}, device_id_type=MESH)

    @pl.loop(1, az_count)
    def _(j):
        pl.semaphore_signal(barrier, inc=1, device_id={"az": (q + j) % az_count}, device_id_type=MESH)

    for g in range(1, groups):
        local(g).start()
    for i in range(n + 3):
        table(i).start()
    pl.semaphore_wait(barrier, rng_count + az_count - 2)

    reach = [i for i in range(len(counts)) if i + 1 < rng_count]
    for g in range(groups):
        for i in reach:
            pl.when(p >= i + 1)(lambda g=g, i=i: halo(g, i).start())
    for copy in small:
        copy.wait()

    def remap(c):
        start, per = chunks[c]
        sub = 2 * per
        out = stage[c].reshape(rows * sub, GW)
        energy = jnp.zeros((8, GW), jnp.float32)
        for gl in range(per):
            g = start + gl
            local(g).wait()
            for i in reach:
                pl.when(p + i + 1 < rng_count)(lambda g=g, i=i: halo(g, i).wait_recv())
            energy = energy + remap_group(
                ext[g].reshape(ext[g].shape[0] * 2, GW), out, sub, gl, blocks,
                lambda b: jnp.maximum(src_ref[b, g] - p * blocks, 0),
                lambda b: off_ref[pl.ds(g, 1), pl.ds(b * BLOCK, BLOCK)],
                lambda t, b: w_ref[t, pl.ds(g, 1), pl.ds(b * BLOCK, BLOCK)],
            )
        recv[c][q] = stage[c][pl.ds(q * piece, piece)]
        return energy

    def spread(send):
        @pl.loop(0, half)
        def _(j):
            send((1 - side) * half + (place + j) % half)

        @pl.loop(1, half)
        def _(j):
            send(side * half + (place + j) % half)

    def send_chunk(c):
        spread(lambda peer: pltpu.make_async_remote_copy(
            src_ref=stage[c].at[pl.ds(peer * piece, piece)],
            dst_ref=recv[c].at[q],
            send_sem=part_send.at[c], recv_sem=part_recv.at[c],
            device_id={"az": peer}, device_id_type=MESH).start())

    def send_last():
        c = n - 1

        @pl.loop(0, subsets)
        def _(r):
            spread(lambda peer: pltpu.make_async_remote_copy(
                src_ref=stage[c].at[pl.ds(peer * piece + r * step, step)],
                dst_ref=recv[c].at[q, pl.ds(r * step, step)],
                send_sem=part_send.at[c], recv_sem=last_recv.at[r],
                device_id={"az": peer}, device_id_type=MESH).start())

    def first_stage(c, r):
        sub = 2 * chunks[c][1]
        flat = recv[c].reshape(az_count * piece * sub, GW)
        x = jnp.concatenate([
            jnp.concatenate(
                [flat[pl.ds((r + k) * sub + s, az_count, stride=piece * sub), :] for s in range(sub)], axis=0)
            for k in range(2)], axis=1)
        x_hi, x_lo = split(x)
        return jnp.dot(
            a_refs[c][...], jnp.concatenate([x_hi, x_lo, x_hi], axis=0), preferred_element_type=jnp.float32)

    def gather_chunk(c):
        table(c).wait()
        others = recv[c].at[pl.ds(0, az_count - 1)]
        pltpu.make_async_copy(others, others, part_recv.at[c]).wait()

        @pl.loop(0, piece // 2)
        def _(i):
            y = first_stage(c, 2 * i)
            y_acc[i] = y if c == 0 else y_acc[i] + y

    def share(src, dst, slot, axis, peer, at):
        return pltpu.make_async_remote_copy(
            src_ref=src, dst_ref=dst.at[slot], send_sem=e_send.at[at],
            recv_sem=e_recv.at[at], device_id={axis: peer}, device_id_type=MESH)

    def share_all(src, dst, slot, axis, count, at):
        dst[slot] = src[...]

        @pl.loop(1, count)
        def _(j):
            share(src, dst, slot, axis, (slot + j) % count, at).start()

    def share_wait(dst, count, at):
        others = dst.at[pl.ds(0, count - 1)]
        pltpu.make_async_copy(others, others, e_send.at[at]).wait()
        pltpu.make_async_copy(others, others, e_recv.at[at]).wait()

    energy = jnp.zeros((8, GW), jnp.float32)
    for c in range(n - 1):
        energy = energy + remap(c)
        send_chunk(c)
        if c >= LAG:
            gather_chunk(c - LAG)
    energy = energy + remap(n - 1)
    e_own[...] = energy
    share_all(e_own, e_az, q, "az", az_count, 0)
    send_last()
    for c in range(max(n - 1 - LAG, 0), n - 1):
        gather_chunk(c)
    share_wait(e_az, az_count, 0)
    e_sum[...] = jnp.sum(e_az[...], axis=0)
    share_all(e_sum, e_rng, p, "rng", rng_count, 1)
    for i in range(n - 1, n + 3):
        table(i).wait()
    share_wait(e_rng, rng_count, 1)
    mean = jnp.sum(jnp.sum(e_rng[...], axis=0), axis=(0, 1), keepdims=True) / cells
    scale = lax.rsqrt(mean + 1e-06)

    halves = total_groups // GW
    nt = (((1,), (1,)), ((), ()))

    @pl.loop(0, subsets)
    def _(s):
        others = recv[n - 1].at[pl.ds(0, az_count - 1), pl.ds(s * step, step)]
        pltpu.make_async_copy(others, others, last_recv.at[s]).wait()
        for k in range(step // 2):
            first = s * step + 2 * k
            y = y_acc[s * (step // 2) + k] + first_stage(n - 1, first)
            t_re, t_im = twist_ref[0], twist_ref[1]
            turned = []
            for i in range(2):
                y_re = y[:total_groups, i * GW:(i + 1) * GW]
                y_im = y[total_groups:, i * GW:(i + 1) * GW]
                turned.append(jnp.concatenate([y_re * t_re - y_im * t_im, y_re * t_im + y_im * t_re], axis=1))
            z_hi, z_lo = split(jnp.concatenate(turned, axis=0) * scale)
            v = (
                lax.dot_general(b_hi_ref[...], z_hi, nt, preferred_element_type=jnp.float32)
                + lax.dot_general(b_hi_ref[...], z_lo, nt, preferred_element_type=jnp.float32)
                + lax.dot_general(b_lo_ref[...], z_hi, nt, preferred_element_type=jnp.float32)
            )
            for i in range(2):
                for c in range(2):
                    for h in range(halves):
                        image_ref[first + i, pl.ds(2 * h + c, GW, stride=2 * halves), :] = (
                            v[c * GW:(c + 1) * GW, i * total_groups + h * GW:i * total_groups + (h + 1) * GW])

    for c in range(n):
        sent = stage[c].at[pl.ds(0, rows - piece)]
        pltpu.make_async_copy(sent, sent, part_send.at[c]).wait()
    for g in range(groups):
        for i in reach:
            pl.when(p >= i + 1)(lambda g=g, i=i: halo(g, i).wait_send())


def fused(spec, src, offsets, weights, tables, chunks, counts, rng_count, az_count):
    rows, groups = spec.shape[:2]
    blocks = rows // BLOCK
    piece = rows // az_count
    step = min(STEP, piece)
    n = len(chunks)
    total_groups = groups * az_count
    cells = float(rows * rng_count * total_groups * GW) * float(total_groups * GW)
    hbm = pl.BlockSpec(memory_space=pl.ANY)
    tile = (8, GW)
    dma = pltpu.SemaphoreType.DMA
    vmem = pltpu.VMEM
    f32 = jnp.float32
    return pl.pallas_call(
        functools.partial(fused_kernel, rows, blocks, groups, chunks, counts, step, cells),
        out_shape=vmem((piece, 2 * total_groups, GW), f32),
        in_specs=[pl.BlockSpec(memory_space=pltpu.SMEM)] + [hbm] * (3 + len(tables)),
        out_specs=pl.BlockSpec(memory_space=vmem),
        scratch_shapes=[vmem((rows + sum(counts), 2, GW), f32)] * groups
        + [vmem((rows, per, 2, GW), f32) for _, per in chunks]
        + [vmem((az_count, piece, per, 2, GW), f32) for _, per in chunks]
        + [vmem(t.shape, t.dtype) for t in tables]
        + [
            vmem((piece // 2, 2 * total_groups, 2 * GW), f32),
            vmem(offsets.shape, offsets.dtype),
            vmem(weights.shape, weights.dtype),
            vmem(tile, f32),
            vmem((az_count,) + tile, f32),
            vmem(tile, f32),
            vmem((rng_count,) + tile, f32),
            dma((2,)),
            dma((len(tables),)),
            dma((groups,)),
            dma((groups, len(counts))),
            dma((groups, len(counts))),
            dma((n,)),
            dma((n,)),
            dma((piece // step,)),
            dma((2,)),
            dma((2,)),
        ],
        compiler_params=pltpu.CompilerParams(
            has_side_effects=True, collective_id=0, vmem_limit_bytes=52 * 1024 * 1024),
    )(src, offsets, weights, spec, *tables)


def store_kernel(parts, band_ref, out_ref, sem):
    size = band_ref.shape[0] // parts
    copies = [
        pltpu.make_async_copy(band_ref.at[pl.ds(i * size, size)], out_ref.at[pl.ds(i * size, size)], sem.at[i])
        for i in range(parts)]
    for copy in copies:
        copy.start()
    for copy in copies:
        copy.wait()


def store(band):
    parts = min(8, band.shape[0])
    return pl.pallas_call(
        functools.partial(store_kernel, parts),
        out_shape=jax.ShapeDtypeStruct(band.shape, band.dtype),
        in_specs=[pl.BlockSpec(memory_space=pltpu.VMEM)],
        out_specs=pl.BlockSpec(memory_space=pl.ANY),
        scratch_shapes=[pltpu.SemaphoreType.DMA((parts,))],
        compiler_params=pltpu.CompilerParams(vmem_limit_bytes=1024 * 1024),
    )(band)


def halo_counts(rows_dev, rng_count):
    total = rows_dev * rng_count
    halo = min(rows_dev - BLOCK + SHIFT_B * BLOCK, total - 2 * BLOCK) + WINDOW - rows_dev
    counts = []
    while halo > 0:
        counts.append(min(halo, rows_dev))
        halo -= rows_dev
    return counts


def body(spectrum, src_block, offsets, tap_weights):
    rows_dev = spectrum.shape[0]
    columns = spectrum.shape[2]
    groups = columns // GW
    rng_count = lax.axis_size("rng")
    az_count = lax.axis_size("az")
    rows_after = rows_dev // az_count
    total_len = columns * az_count
    chunks = plan(groups)
    tables = [jnp.asarray(t) for t in dft_tables(az_count, groups, chunks)]
    spec = spectrum.reshape(rows_dev, 2, groups, GW).transpose(0, 2, 1, 3)
    counts = halo_counts(rows_dev, rng_count)
    band = fused(spec, src_block.T, offsets, tap_weights, tables, chunks, counts, rng_count, az_count)
    image = store(band)
    return (
        image.reshape(rows_after, total_len // GW, 2, GW)
        .transpose(0, 2, 1, 3)
        .reshape(rows_after, 2, total_len)
    )


def solution(mesh):
    placed = (P("rng", None, "az"), P("az", "rng"), P("az", "rng"), P(None, "az", "rng"))
    return jax.shard_map(
        body, mesh=mesh, in_specs=placed, out_specs=P(("rng", "az"), None, None), check_vma=False
    )
```

```python
import functools

import jax
import jax.numpy as jnp
import numpy as np
from jax import lax
from jax.experimental import pallas as pl
from jax.experimental.pallas import tpu as pltpu
from jax.sharding import PartitionSpec as P

BLOCK = 128
GW = 128
TAPS = 8
SHIFT_B = 5
WINDOW = 144
LAG = 2
STEP = 4

MESH = pl.DeviceIdType.MESH


def split_np(x):
    hi = x.astype(jnp.bfloat16)
    lo = (x - hi.astype(np.float64)).astype(jnp.bfloat16)
    return hi, lo


def split(x):
    hi = x.astype(jnp.bfloat16)
    lo = (x - hi.astype(jnp.float32)).astype(jnp.bfloat16)
    return hi, lo


def plan(groups):
    last = max(1, groups // 4)
    single = min(groups - last, (3 * groups) // 8)
    sizes = ([1, 1] if single else []) + [2] * (single - 1)
    left = groups - last - single
    sizes += [4] * (left // 2) + [2] * (left % 2) + [2 * last]
    starts = [sum(sizes[:i]) for i in range(len(sizes))]
    return tuple(zip(starts, sizes))


def units_of(chunks):
    units = []
    for c, (start, size) in enumerate(chunks):
        width = min(size, 2)
        units += [(c, at, width) for at in range(0, size, width)]
    return tuple(units)


def dft_tables(az_count, groups, chunks):
    total_groups = az_count * groups
    total_len = total_groups * GW
    k1 = np.arange(total_groups)
    gl, az = np.meshgrid(np.arange(groups), np.arange(az_count), indexing="ij")
    angle = 2.0 * np.pi * ((k1[:, None, None] * (az * groups + gl)[None]) % total_groups) / total_groups
    first = np.empty((2, total_groups, groups, 2, az_count))
    first[0, :, :, 0] = np.cos(angle)
    first[0, :, :, 1] = -np.sin(angle)
    first[1, :, :, 0] = np.sin(angle)
    first[1, :, :, 1] = np.cos(angle)
    first = first.reshape(2 * total_groups, 2 * groups, az_count)
    stage_one = []
    for start, size in chunks:
        hi, lo = split_np(first[:, start:start + size].reshape(2 * total_groups, size * az_count))
        stage_one.append(np.concatenate([hi, hi, lo], axis=1))
    l = np.arange(GW)
    turn = 2.0 * np.pi * (k1[:, None] * l[None, :]) / total_len
    twist = np.stack([np.cos(turn), np.sin(turn)]).astype(np.float32) / np.float32(total_len)
    inner = 2.0 * np.pi * ((l[:, None] * l[None, :]) % GW) / GW
    second = np.empty((2, GW, 2, GW))
    second[0, :, 0] = np.cos(inner)
    second[0, :, 1] = -np.sin(inner)
    second[1, :, 0] = np.sin(inner)
    second[1, :, 1] = np.cos(inner)
    b_hi, b_lo = split_np(second.reshape(2 * GW, 2 * GW))
    return stage_one + [twist, b_hi, b_lo]


def remap_block(ext, width, out, sub, at, b, src, off, weight_row):
    source = [ext[pl.ds(src * (BLOCK * width) + c, WINDOW, stride=width), :] for c in range(width)]
    source = jnp.concatenate(source, axis=1) if width > 1 else source[0]
    where = lax.broadcasted_iota(jnp.int32, (WINDOW, BLOCK), 0) - off
    taps = jnp.zeros((WINDOW, BLOCK), jnp.float32)
    for t in range(TAPS):
        taps = jnp.where(where == t, weight_row(t), taps)
    t_hi, t_lo = split(taps)
    s_hi, s_lo = split(source)
    left = jnp.concatenate([t_hi, t_lo, t_hi], axis=0)
    right = jnp.concatenate([s_hi, s_hi, s_lo], axis=0)
    value = lax.dot_general(
        left, right, (((0,), (0,)), ((), ())), preferred_element_type=jnp.float32
    )
    energy = jnp.zeros((8, GW), jnp.float32)
    for c in range(width):
        half = value[:, c * GW:(c + 1) * GW]
        out[pl.ds(b * BLOCK * sub + at + c, BLOCK, stride=sub), :] = half
        energy = energy + jnp.sum((half * half).reshape(BLOCK // 8, 8, GW), axis=0)
    return energy


def first_stage(recv, a_ref, sub, piece, az_count, row, stored_rows):
    flat = recv.reshape(az_count * stored_rows * sub, GW)
    x = jnp.concatenate([
        jnp.concatenate(
            [flat[pl.ds((row + k) * sub + s, az_count, stride=stored_rows * sub), :] for s in range(sub)], axis=0)
        for k in range(2)], axis=1)
    x_hi, x_lo = split(x)
    return jnp.dot(
        a_ref[...], jnp.concatenate([x_hi, x_lo, x_hi], axis=0), preferred_element_type=jnp.float32)


def second_stage(y, scale, twist_ref, b_hi_ref, b_lo_ref, store):
    total_groups = y.shape[0] // 2
    halves = total_groups // GW
    nt = (((1,), (1,)), ((), ()))
    t_re, t_im = twist_ref[0], twist_ref[1]
    turned = []
    for i in range(2):
        y_re = y[:total_groups, i * GW:(i + 1) * GW]
        y_im = y[total_groups:, i * GW:(i + 1) * GW]
        turned.append(jnp.concatenate([y_re * t_re - y_im * t_im, y_re * t_im + y_im * t_re], axis=1))
    z_hi, z_lo = split(jnp.concatenate(turned, axis=0) * scale)
    v = (
        lax.dot_general(b_hi_ref[...], z_hi, nt, preferred_element_type=jnp.float32)
        + lax.dot_general(b_hi_ref[...], z_lo, nt, preferred_element_type=jnp.float32)
        + lax.dot_general(b_lo_ref[...], z_hi, nt, preferred_element_type=jnp.float32)
    )
    for i in range(2):
        for c in range(2):
            for h in range(halves):
                store(i, pl.ds(2 * h + c, GW, stride=2 * halves),
                      v[c * GW:(c + 1) * GW, i * total_groups + h * GW:i * total_groups + (h + 1) * GW])


def fused_kernel(rows, blocks, chunks, units, counts, step, cells, src_hbm, off_hbm, w_hbm, spec_ref, *rest):
    n = len(chunks)
    tables_hbm, rest = rest[:n + 3], rest[n + 3:]
    image_ref, y_acc, last_recv_ref, scale_ref, a_last, twist_ref, b_hi_ref, b_lo_ref = rest[:8]
    scratch = rest[8:]
    ext, scratch = scratch[:len(units)], scratch[len(units):]
    stage, scratch = scratch[:n], scratch[n:]
    recv, scratch = scratch[:n - 1] + (last_recv_ref,), scratch[n - 1:]
    a_refs, scratch = scratch[:n - 1] + (a_last,), scratch[n - 1:]
    tables = a_refs + (twist_ref, b_hi_ref, b_lo_ref)
    (src_ref, off_ref, w_ref, e_own, e_az, e_sum, e_rng, small_sem, table_sem, local_sem, halo_send, halo_recv,
     part_send, part_recv, last_recv, e_send, e_recv) = scratch
    rng_count, az_count = lax.axis_size("rng"), lax.axis_size("az")
    p, q = lax.axis_index("rng"), lax.axis_index("az")
    piece = rows // az_count
    half = max(az_count // 2, 1)
    side, place = q // half, q % half
    subsets = piece // step
    reach = [i for i in range(len(counts)) if i + 1 < rng_count]

    barrier = pltpu.get_barrier_semaphore()

    @pl.loop(1, rng_count)
    def _(j):
        pl.semaphore_signal(barrier, inc=1, device_id={"rng": (p + j) % rng_count}, device_id_type=MESH)

    @pl.loop(1, az_count)
    def _(j):
        pl.semaphore_signal(barrier, inc=1, device_id={"az": (q + j) % az_count}, device_id_type=MESH)

    def column(u):
        c, at, width = units[u]
        return pl.ds(chunks[c][0] + at, width)

    def local(u):
        return pltpu.make_async_copy(
            spec_ref.at[:, column(u)], ext[u].at[pl.ds(0, rows)], local_sem.at[u])

    def halo(u, i):
        source = ext[u].at[pl.ds(0, counts[i])] if u == 0 else spec_ref.at[pl.ds(0, counts[i]), column(u)]
        return pltpu.make_async_remote_copy(
            src_ref=source,
            dst_ref=ext[u].at[pl.ds(rows + sum(counts[:i]), counts[i])],
            send_sem=halo_send.at[u, i], recv_sem=halo_recv.at[u, i],
            device_id={"rng": (p + rng_count - i - 1) % rng_count}, device_id_type=MESH)

    def table(i):
        return pltpu.make_async_copy(tables_hbm[i], tables[i], table_sem.at[i])

    local(0).start()
    small = [pltpu.make_async_copy(hbm, ref, small_sem.at[i])
             for i, (hbm, ref) in enumerate(((src_hbm, src_ref), (off_hbm, off_ref), (w_hbm, w_ref)))]
    for copy in small:
        copy.start()
    for u in range(1, len(units)):
        local(u).start()
    for i in range(n + 3):
        table(i).start()
    local(0).wait()
    pl.semaphore_wait(barrier, rng_count + az_count - 2)

    for u in range(len(units)):
        for i in reach:
            pl.when(p >= i + 1)(lambda u=u, i=i: halo(u, i).start())
    for copy in small:
        copy.wait()

    def arrive(u):
        if u:
            local(u).wait()
        for i in reach:
            pl.when(p + i + 1 < rng_count)(lambda: halo(u, i).wait_recv())

    def remap(u, b):
        c, at, width = units[u]
        g, sub = (chunks[c][0] + at) // 2, chunks[c][1]
        lanes = pl.ds(b * BLOCK if isinstance(b, int) else pl.multiple_of(b * BLOCK, BLOCK), BLOCK)
        return remap_block(
            ext[u].reshape(ext[u].shape[0] * width, GW), width, stage[c].reshape(rows * sub, GW), sub, at, b,
            jnp.maximum(src_ref[b, g] - p * blocks, 0), off_ref[pl.ds(g, 1), lanes],
            lambda t: w_ref[t, pl.ds(g, 1), lanes])

    def keep(c):
        recv[c][q] = stage[c][pl.ds(q * piece, piece)]

    def remap_chunk(c):
        energy = jnp.zeros((8, GW), jnp.float32)
        for u in range(len(units)):
            if units[u][0] == c:
                arrive(u)
                for b in range(blocks):
                    energy = energy + remap(u, b)
        keep(c)
        return energy

    def spread(send):
        @pl.loop(0, half)
        def _(j):
            send((1 - side) * half + (place + j) % half)

        @pl.loop(1, half)
        def _(j):
            send(side * half + (place + j) % half)

    def send_piece(c, peer):
        pltpu.make_async_remote_copy(
            src_ref=stage[c].at[pl.ds(peer * piece, piece)],
            dst_ref=recv[c].at[q],
            send_sem=part_send.at[c], recv_sem=part_recv.at[c],
            device_id={"az": peer}, device_id_type=MESH).start()

    def first_chunk():
        peers = BLOCK // piece
        energy = jnp.zeros((8, GW), jnp.float32)
        arrive(0)
        for k in range(blocks):
            b = (k + (1 - side) * (blocks // 2)) % blocks
            energy = energy + remap(0, b)

            @pl.loop(0, peers)
            def _(j):
                peer = b * peers + (place + j) % peers
                pl.when(peer != q)(lambda: send_piece(0, peer))

        keep(0)
        return energy

    def send_last():
        c = n - 1

        @pl.loop(0, subsets)
        def _(r):
            spread(lambda peer: pltpu.make_async_remote_copy(
                src_ref=stage[c].at[pl.ds(peer * piece + r * step, step)],
                dst_ref=recv[c].at[q, pl.ds(r * step, step)],
                send_sem=part_send.at[c], recv_sem=last_recv.at[r],
                device_id={"az": peer}, device_id_type=MESH).start())

    def rows_of(c, row):
        return first_stage(recv[c], a_refs[c], chunks[c][1], piece, az_count, row, piece)

    def gather_chunk(c):
        table(c).wait()
        others = recv[c].at[pl.ds(0, az_count - 1)]
        pltpu.make_async_copy(others, others, part_recv.at[c]).wait()

        @pl.loop(0, piece // 2)
        def _(i):
            y = rows_of(c, 2 * i)
            y_acc[i] = y if c == 0 else y_acc[i] + y

    def share(src, dst, slot, axis, peer, at):
        return pltpu.make_async_remote_copy(
            src_ref=src, dst_ref=dst.at[slot], send_sem=e_send.at[at],
            recv_sem=e_recv.at[at], device_id={axis: peer}, device_id_type=MESH)

    def share_all(src, dst, slot, axis, count, at):
        dst[slot] = src[...]

        @pl.loop(1, count)
        def _(j):
            share(src, dst, slot, axis, (slot + j) % count, at).start()

    def share_wait(dst, count, at):
        others = dst.at[pl.ds(0, count - 1)]
        pltpu.make_async_copy(others, others, e_send.at[at]).wait()
        pltpu.make_async_copy(others, others, e_recv.at[at]).wait()

    energy = first_chunk()
    for c in range(1, n - 1):
        energy = energy + remap_chunk(c)
        spread(functools.partial(send_piece, c))
        if c >= LAG:
            gather_chunk(c - LAG)
    energy = energy + remap_chunk(n - 1)
    e_own[...] = energy
    share_all(e_own, e_az, q, "az", az_count, 0)
    send_last()
    for c in range(max(n - 1 - LAG, 0), n - 1):
        gather_chunk(c)
    share_wait(e_az, az_count, 0)
    e_sum[...] = jnp.sum(e_az[...], axis=0)
    share_all(e_sum, e_rng, p, "rng", rng_count, 1)
    for i in range(n - 1, n + 3):
        table(i).wait()
    share_wait(e_rng, rng_count, 1)
    mean = jnp.sum(jnp.sum(e_rng[...], axis=0), axis=(0, 1), keepdims=True) / cells
    scale = lax.rsqrt(mean + 1e-06)
    scale_ref[...] = jnp.broadcast_to(scale, scale_ref.shape)

    def arrived(s):
        others = recv[n - 1].at[pl.ds(0, az_count - 1), pl.ds(s * step, step)]
        pltpu.make_async_copy(others, others, last_recv.at[s]).wait()

    @pl.loop(0, subsets - 1)
    def _(s):
        arrived(s)
        for k in range(step // 2):
            first = s * step + 2 * k
            y = y_acc[s * (step // 2) + k] + rows_of(n - 1, first)

            def store(i, lines, value):
                image_ref[first + i, lines, :] = value

            second_stage(y, scale, twist_ref, b_hi_ref, b_lo_ref, store)

    for c in range(n):
        sent = stage[c].at[pl.ds(0, rows - piece)]
        pltpu.make_async_copy(sent, sent, part_send.at[c]).wait()
    for u in range(len(units)):
        for i in reach:
            pl.when(p >= i + 1)(lambda u=u, i=i: halo(u, i).wait_send())
    arrived(subsets - 1)


def fused(spec, src, offsets, weights, tables, chunks, counts, step, rng_count, az_count):
    rows, columns = spec.shape[:2]
    blocks = rows // BLOCK
    piece = rows // az_count
    n = len(chunks)
    units = units_of(chunks)
    total_groups = columns // 2 * az_count
    cells = float(rows * rng_count * total_groups * GW) * float(total_groups * GW)
    hbm = pl.BlockSpec(memory_space=pl.ANY)
    tile = (8, GW)
    dma = pltpu.SemaphoreType.DMA
    vmem = pltpu.VMEM
    f32 = jnp.float32
    sizes = [size for _, size in chunks]
    outs = [
        vmem(((piece - step), 2 * total_groups, GW), f32),
        vmem((piece // 2, 2 * total_groups, 2 * GW), f32),
        vmem((az_count, piece, sizes[-1], 1, GW), f32),
        vmem(tile, f32),
    ] + [vmem(t.shape, t.dtype) for t in tables[n - 1:]]
    return pl.pallas_call(
        functools.partial(fused_kernel, rows, blocks, chunks, units, counts, step, cells),
        out_shape=outs,
        in_specs=[hbm] * (4 + len(tables)),
        out_specs=[pl.BlockSpec(memory_space=vmem)] * len(outs),
        scratch_shapes=[vmem((rows + sum(counts), width, 1, GW), f32) for _, _, width in units]
        + [vmem((rows, size, 1, GW), f32) for size in sizes]
        + [vmem((az_count, piece, size, 1, GW), f32) for size in sizes[:-1]]
        + [vmem(t.shape, t.dtype) for t in tables[:n - 1]]
        + [
            pltpu.SMEM(src.shape, src.dtype),
            vmem(offsets.shape, offsets.dtype),
            vmem(weights.shape, weights.dtype),
            vmem(tile, f32),
            vmem((az_count,) + tile, f32),
            vmem(tile, f32),
            vmem((rng_count,) + tile, f32),
            dma((3,)),
            dma((len(tables),)),
            dma((len(units),)),
            dma((len(units), len(counts))),
            dma((len(units), len(counts))),
            dma((n,)),
            dma((n,)),
            dma((piece // step,)),
            dma((2,)),
            dma((2,)),
        ],
        compiler_params=pltpu.CompilerParams(
            has_side_effects=True, collective_id=0, vmem_limit_bytes=40 * 1024 * 1024),
    )(src, offsets, weights, spec, *tables)


def store_kernel(step, band_ref, y_acc, recv, scale_ref, a_ref, twist_ref, b_hi_ref, b_lo_ref, out_ref, end, sem):
    done = band_ref.shape[0]
    parts = done // step
    az_count, piece, sub = recv.shape[:3]

    def copy(i):
        source = band_ref.at[pl.ds(i * step, step)] if i < parts else end
        return pltpu.make_async_copy(source, out_ref.at[pl.ds(i * step, step)], sem.at[i])

    for i in range(parts):
        copy(i).start()
    for k in range(step // 2):
        first = done + 2 * k
        y = y_acc[first // 2] + first_stage(recv, a_ref, sub, piece, az_count, first, piece)

        def store(i, lines, value, k=k):
            end[2 * k + i, lines, :] = value

        second_stage(y, scale_ref[:1, :1], twist_ref, b_hi_ref, b_lo_ref, store)
    copy(parts).start()
    for i in range(parts + 1):
        copy(i).wait()


def store(step, rows, band, *rest):
    parts = rows // step
    vmem = pltpu.VMEM
    return pl.pallas_call(
        functools.partial(store_kernel, step),
        out_shape=jax.ShapeDtypeStruct((rows,) + band.shape[1:], band.dtype),
        in_specs=[pl.BlockSpec(memory_space=vmem)] * (1 + len(rest)),
        out_specs=pl.BlockSpec(memory_space=pl.ANY),
        scratch_shapes=[vmem((step,) + band.shape[1:], band.dtype), pltpu.SemaphoreType.DMA((parts,))],
        compiler_params=pltpu.CompilerParams(vmem_limit_bytes=12 * 1024 * 1024),
    )(band, *rest)


def halo_counts(rows_dev, rng_count):
    total = rows_dev * rng_count
    halo = min(rows_dev - BLOCK + SHIFT_B * BLOCK, total - 2 * BLOCK) + WINDOW - rows_dev
    counts = []
    while halo > 0:
        counts.append(min(halo, rows_dev))
        halo -= rows_dev
    return counts


def body(spectrum, src_block, offsets, tap_weights):
    rows_dev = spectrum.shape[0]
    columns = spectrum.shape[2]
    groups = columns // GW
    rng_count = lax.axis_size("rng")
    az_count = lax.axis_size("az")
    rows_after = rows_dev // az_count
    total_len = columns * az_count
    chunks = plan(groups)
    tables = [jnp.asarray(t) for t in dft_tables(az_count, groups, chunks)]
    spec = spectrum.reshape(rows_dev, 2, groups, GW).transpose(0, 2, 1, 3).reshape(rows_dev, 2 * groups, 1, GW)
    counts = halo_counts(rows_dev, rng_count)
    step = min(STEP, rows_after // 2)
    held = fused(spec, src_block.T, offsets, tap_weights, tables, chunks, counts, step, rng_count, az_count)
    image = store(step, rows_after, *held)
    return (
        image.reshape(rows_after, total_len // GW, 2, GW)
        .transpose(0, 2, 1, 3)
        .reshape(rows_after, 2, total_len)
    )


def solution(mesh):
    placed = (P("rng", None, "az"), P("az", "rng"), P("az", "rng"), P(None, "az", "rng"))
    return jax.shard_map(
        body, mesh=mesh, in_specs=placed, out_specs=P(("rng", "az"), None, None), check_vma=False
    )
```

```python
import functools

import jax
import jax.numpy as jnp
import numpy as np
from jax import lax
from jax.experimental import pallas as pl
from jax.experimental.pallas import tpu as pltpu
from jax.sharding import PartitionSpec as P

BLOCK = 128
GW = 128
TAPS = 8
SHIFT_B = 5
WINDOW = 144
LAG = 2
RELAY = 1
RELAY_AT = 4
STEP = 4

MESH = pl.DeviceIdType.MESH


def split_np(x):
    hi = x.astype(jnp.bfloat16)
    lo = (x - hi.astype(np.float64)).astype(jnp.bfloat16)
    return hi, lo


def split(x):
    hi = x.astype(jnp.bfloat16)
    lo = (x - hi.astype(jnp.float32)).astype(jnp.bfloat16)
    return hi, lo


def plan(groups):
    last = max(1, groups // 4)
    single = min(groups - last, (3 * groups) // 8)
    sizes = ([1, 1] if single else []) + [2] * (single - 1)
    left = groups - last - single
    sizes += [4] * (left // 2) + [2] * (left % 2) + [2 * last]
    starts = [sum(sizes[:i]) for i in range(len(sizes))]
    return tuple(zip(starts, sizes))


def units_of(chunks):
    units = []
    for c, (start, size) in enumerate(chunks):
        width = min(size, 2)
        units += [(c, at, width) for at in range(0, size, width)]
    return tuple(units)


def dft_tables(az_count, groups, chunks):
    total_groups = az_count * groups
    total_len = total_groups * GW
    k1 = np.arange(total_groups)
    gl, az = np.meshgrid(np.arange(groups), np.arange(az_count), indexing="ij")
    angle = 2.0 * np.pi * ((k1[:, None, None] * (az * groups + gl)[None]) % total_groups) / total_groups
    first = np.empty((2, total_groups, groups, 2, az_count))
    first[0, :, :, 0] = np.cos(angle)
    first[0, :, :, 1] = -np.sin(angle)
    first[1, :, :, 0] = np.sin(angle)
    first[1, :, :, 1] = np.cos(angle)
    first = first.reshape(2 * total_groups, 2 * groups, az_count)
    stage_one = []
    for start, size in chunks:
        hi, lo = split_np(first[:, start:start + size].reshape(2 * total_groups, size * az_count))
        stage_one.append(np.concatenate([hi, hi, lo], axis=1))
    l = np.arange(GW)
    turn = 2.0 * np.pi * (k1[:, None] * l[None, :]) / total_len
    twist = np.stack([np.cos(turn), np.sin(turn)]).astype(np.float32) / np.float32(total_len)
    inner = 2.0 * np.pi * ((l[:, None] * l[None, :]) % GW) / GW
    second = np.empty((2, GW, 2, GW))
    second[0, :, 0] = np.cos(inner)
    second[0, :, 1] = -np.sin(inner)
    second[1, :, 0] = np.sin(inner)
    second[1, :, 1] = np.cos(inner)
    b_hi, b_lo = split_np(second.reshape(2 * GW, 2 * GW))
    return stage_one + [twist, b_hi, b_lo]


def remap_block(ext, width, out, sub, at, b, src, off, weight_row):
    source = [ext[pl.ds(src * (BLOCK * width) + c, WINDOW, stride=width), :] for c in range(width)]
    source = jnp.concatenate(source, axis=1) if width > 1 else source[0]
    where = lax.broadcasted_iota(jnp.int32, (WINDOW, BLOCK), 0) - off
    taps = jnp.zeros((WINDOW, BLOCK), jnp.float32)
    for t in range(TAPS):
        taps = jnp.where(where == t, weight_row(t), taps)
    t_hi, t_lo = split(taps)
    s_hi, s_lo = split(source)
    left = jnp.concatenate([t_hi, t_lo, t_hi], axis=0)
    right = jnp.concatenate([s_hi, s_hi, s_lo], axis=0)
    value = lax.dot_general(
        left, right, (((0,), (0,)), ((), ())), preferred_element_type=jnp.float32
    )
    energy = jnp.zeros((8, GW), jnp.float32)
    for c in range(width):
        half = value[:, c * GW:(c + 1) * GW]
        out[pl.ds(b * BLOCK * sub + at + c, BLOCK, stride=sub), :] = half
        energy = energy + jnp.sum((half * half).reshape(BLOCK // 8, 8, GW), axis=0)
    return energy


def first_stage(recv, a_ref, sub, piece, az_count, row, stored_rows):
    flat = recv.reshape(az_count * stored_rows * sub, GW)
    x = jnp.concatenate([
        jnp.concatenate(
            [flat[pl.ds((row + k) * sub + s, az_count, stride=stored_rows * sub), :] for s in range(sub)], axis=0)
        for k in range(2)], axis=1)
    x_hi, x_lo = split(x)
    return jnp.dot(
        a_ref[...], jnp.concatenate([x_hi, x_lo, x_hi], axis=0), preferred_element_type=jnp.float32)


def second_stage(y, scale, twist_ref, b_hi_ref, b_lo_ref, store):
    total_groups = y.shape[0] // 2
    halves = total_groups // GW
    nt = (((1,), (1,)), ((), ()))
    t_re, t_im = twist_ref[0], twist_ref[1]
    turned = []
    for i in range(2):
        y_re = y[:total_groups, i * GW:(i + 1) * GW]
        y_im = y[total_groups:, i * GW:(i + 1) * GW]
        turned.append(jnp.concatenate([y_re * t_re - y_im * t_im, y_re * t_im + y_im * t_re], axis=1))
    z_hi, z_lo = split(jnp.concatenate(turned, axis=0) * scale)
    v = (
        lax.dot_general(b_hi_ref[...], z_hi, nt, preferred_element_type=jnp.float32)
        + lax.dot_general(b_hi_ref[...], z_lo, nt, preferred_element_type=jnp.float32)
        + lax.dot_general(b_lo_ref[...], z_hi, nt, preferred_element_type=jnp.float32)
    )
    for i in range(2):
        for c in range(2):
            for h in range(halves):
                store(i, pl.ds(2 * h + c, GW, stride=2 * halves),
                      v[c * GW:(c + 1) * GW, i * total_groups + h * GW:i * total_groups + (h + 1) * GW])


def fused_kernel(rows, blocks, chunks, units, counts, step, cells, src_hbm, off_hbm, w_hbm, spec_ref, *rest):
    n = len(chunks)
    tables_hbm, rest = rest[:n + 3], rest[n + 3:]
    image_ref, y_acc, last_recv_ref, scale_ref, a_last, twist_ref, b_hi_ref, b_lo_ref = rest[:8]
    scratch = rest[8:]
    ext, scratch = scratch[:len(units)], scratch[len(units):]
    stage, scratch = scratch[:n], scratch[n:]
    recv, scratch = scratch[:n - 1] + (last_recv_ref,), scratch[n - 1:]
    a_refs, scratch = scratch[:n - 1] + (a_last,), scratch[n - 1:]
    tables = a_refs + (twist_ref, b_hi_ref, b_lo_ref)
    (src_ref, off_ref, w_ref, e_own, e_az, e_sum, e_rng, small_sem, table_sem, local_sem, halo_send, halo_recv,
     part_send, part_recv, last_recv, e_send, e_recv, relay_sem, *relay) = scratch
    rng_count, az_count = lax.axis_size("rng"), lax.axis_size("az")
    p, q = lax.axis_index("rng"), lax.axis_index("az")
    piece = rows // az_count
    half = max(az_count // 2, 1)
    side, place = q // half, q % half
    subsets = piece // step
    reach = [i for i in range(len(counts)) if i + 1 < rng_count]

    barrier = pltpu.get_barrier_semaphore()

    @pl.loop(1, rng_count)
    def _(j):
        pl.semaphore_signal(barrier, inc=1, device_id={"rng": (p + j) % rng_count}, device_id_type=MESH)

    @pl.loop(1, az_count)
    def _(j):
        pl.semaphore_signal(barrier, inc=1, device_id={"az": (q + j) % az_count}, device_id_type=MESH)

    def column(u):
        c, at, width = units[u]
        return pl.ds(chunks[c][0] + at, width)

    def local(u):
        return pltpu.make_async_copy(
            spec_ref.at[:, column(u)], ext[u].at[pl.ds(0, rows)], local_sem.at[u])

    def halo(u, i):
        source = ext[u].at[pl.ds(0, counts[i])] if u == 0 else spec_ref.at[pl.ds(0, counts[i]), column(u)]
        return pltpu.make_async_remote_copy(
            src_ref=source,
            dst_ref=ext[u].at[pl.ds(rows + sum(counts[:i]), counts[i])],
            send_sem=halo_send.at[u, i], recv_sem=halo_recv.at[u, i],
            device_id={"rng": (p + rng_count - i - 1) % rng_count}, device_id_type=MESH)

    def table(i):
        return pltpu.make_async_copy(tables_hbm[i], tables[i], table_sem.at[i])

    local(0).start()
    small = [pltpu.make_async_copy(hbm, ref, small_sem.at[i])
             for i, (hbm, ref) in enumerate(((src_hbm, src_ref), (off_hbm, off_ref), (w_hbm, w_ref)))]
    for copy in small:
        copy.start()
    local(0).wait()
    pl.semaphore_wait(barrier, rng_count + az_count - 2)

    for u in range(len(units)):
        for i in reach:
            pl.when(p >= i + 1)(lambda u=u, i=i: halo(u, i).start())
    for u in range(1, len(units)):
        local(u).start()
    for i in range(n + 3):
        table(i).start()
    for copy in small:
        copy.wait()

    def arrive(u):
        if u:
            local(u).wait()
        for i in reach:
            pl.when(p + i + 1 < rng_count)(lambda: halo(u, i).wait_recv())

    def remap(u, b):
        c, at, width = units[u]
        g, sub = (chunks[c][0] + at) // 2, chunks[c][1]
        lanes = pl.ds(b * BLOCK if isinstance(b, int) else pl.multiple_of(b * BLOCK, BLOCK), BLOCK)
        return remap_block(
            ext[u].reshape(ext[u].shape[0] * width, GW), width, stage[c].reshape(rows * sub, GW), sub, at, b,
            jnp.maximum(src_ref[b, g] - p * blocks, 0), off_ref[pl.ds(g, 1), lanes],
            lambda t: w_ref[t, pl.ds(g, 1), lanes])

    def keep(c):
        recv[c][q] = stage[c][pl.ds(q * piece, piece)]

    def remap_chunk(c):
        energy = jnp.zeros((8, GW), jnp.float32)
        for u in range(len(units)):
            if units[u][0] == c:
                arrive(u)
                for b in range(blocks):
                    energy = energy + remap(u, b)
        keep(c)
        return energy

    def spread(send):
        @pl.loop(0, half)
        def _(j):
            send((1 - side) * half + (place + j) % half)

        @pl.loop(1, half)
        def _(j):
            send(side * half + (place + j) % half)

    def send_piece(c, peer):
        pltpu.make_async_remote_copy(
            src_ref=stage[c].at[pl.ds(peer * piece, piece)],
            dst_ref=recv[c].at[q],
            send_sem=part_send.at[c], recv_sem=part_recv.at[c],
            device_id={"az": peer}, device_id_type=MESH).start()

    def hand_over(peer):
        pltpu.make_async_remote_copy(
            src_ref=stage[RELAY].at[pl.ds(peer * piece, piece)],
            dst_ref=relay[0].at[peer % half // 2],
            send_sem=relay_sem.at[0], recv_sem=relay_sem.at[1],
            device_id={"rng": 1 - p}, device_id_type=MESH).start()

    def send_relayed():
        @pl.loop(0, half)
        def _(j):
            peer = (1 - side) * half + (place + j) % half
            via = (p == 0) & (peer % 2 == 0)
            pl.when(via)(lambda: hand_over(peer))
            pl.when(jnp.logical_not(via))(lambda: send_piece(RELAY, peer))

        @pl.loop(1, half)
        def _(j):
            send_piece(RELAY, side * half + (place + j) % half)

    def forward():
        pltpu.make_async_copy(relay[0], relay[0], relay_sem.at[1]).wait()

        @pl.loop(0, half // 2)
        def _(i):
            pltpu.make_async_remote_copy(
                src_ref=relay[0].at[i],
                dst_ref=recv[RELAY].at[q],
                send_sem=relay_sem.at[2], recv_sem=part_recv.at[RELAY],
                device_id={"rng": 1 - p, "az": (1 - side) * half + 2 * i}, device_id_type=MESH).start()

    def relay_done():
        def handed():
            sent = stage[RELAY].at[pl.ds(0, rows - piece - half // 2 * piece)]
            pltpu.make_async_copy(sent, sent, part_send.at[RELAY]).wait()
            pltpu.make_async_copy(relay[0], relay[0], relay_sem.at[0]).wait()

        def forwarded():
            sent = stage[RELAY].at[pl.ds(0, rows - piece)]
            pltpu.make_async_copy(sent, sent, part_send.at[RELAY]).wait()
            pltpu.make_async_copy(relay[0], relay[0], relay_sem.at[2]).wait()

        pl.when(p == 0)(handed)
        pl.when(p != 0)(forwarded)

    def first_chunk():
        peers = BLOCK // piece
        energy = jnp.zeros((8, GW), jnp.float32)
        arrive(0)
        for k in range(blocks):
            b = (k + (1 - side) * (blocks // 2)) % blocks
            energy = energy + remap(0, b)

            @pl.loop(0, peers)
            def _(j):
                peer = b * peers + (place + j) % peers
                pl.when(peer != q)(lambda: send_piece(0, peer))

        keep(0)
        return energy

    def send_last():
        c = n - 1

        @pl.loop(0, subsets)
        def _(r):
            spread(lambda peer: pltpu.make_async_remote_copy(
                src_ref=stage[c].at[pl.ds(peer * piece + r * step, step)],
                dst_ref=recv[c].at[q, pl.ds(r * step, step)],
                send_sem=part_send.at[c], recv_sem=last_recv.at[r],
                device_id={"az": peer}, device_id_type=MESH).start())

    def rows_of(c, row):
        return first_stage(recv[c], a_refs[c], chunks[c][1], piece, az_count, row, piece)

    def gather_chunk(c):
        table(c).wait()
        others = recv[c].at[pl.ds(0, az_count - 1)]
        pltpu.make_async_copy(others, others, part_recv.at[c]).wait()

        @pl.loop(0, piece // 2)
        def _(i):
            y = rows_of(c, 2 * i)
            y_acc[i] = y if c == 0 else y_acc[i] + y

    def share(src, dst, slot, axis, peer, at):
        return pltpu.make_async_remote_copy(
            src_ref=src, dst_ref=dst.at[slot], send_sem=e_send.at[at],
            recv_sem=e_recv.at[at], device_id={axis: peer}, device_id_type=MESH)

    def share_all(src, dst, slot, axis, count, at):
        dst[slot] = src[...]

        @pl.loop(1, count)
        def _(j):
            share(src, dst, slot, axis, (slot + j) % count, at).start()

    def share_wait(dst, count, at):
        others = dst.at[pl.ds(0, count - 1)]
        pltpu.make_async_copy(others, others, e_send.at[at]).wait()
        pltpu.make_async_copy(others, others, e_recv.at[at]).wait()

    energy = first_chunk()
    for c in range(1, n - 1):
        energy = energy + remap_chunk(c)
        if relay and c == RELAY:
            send_relayed()
        else:
            spread(functools.partial(send_piece, c))
        if c >= LAG and not (relay and c - LAG == RELAY):
            gather_chunk(c - LAG)
        if relay and c == RELAY_AT:
            pl.when(p != 0)(forward)
    energy = energy + remap_chunk(n - 1)
    e_own[...] = energy
    share_all(e_own, e_az, q, "az", az_count, 0)
    send_last()
    for c in range(max(n - 1 - LAG, 0), n - 1):
        gather_chunk(c)
    if relay:
        gather_chunk(RELAY)
    share_wait(e_az, az_count, 0)
    e_sum[...] = jnp.sum(e_az[...], axis=0)
    share_all(e_sum, e_rng, p, "rng", rng_count, 1)
    for i in range(n - 1, n + 3):
        table(i).wait()
    share_wait(e_rng, rng_count, 1)
    mean = jnp.sum(jnp.sum(e_rng[...], axis=0), axis=(0, 1), keepdims=True) / cells
    scale = lax.rsqrt(mean + 1e-06)
    scale_ref[...] = jnp.broadcast_to(scale, scale_ref.shape)

    def arrived(s):
        others = recv[n - 1].at[pl.ds(0, az_count - 1), pl.ds(s * step, step)]
        pltpu.make_async_copy(others, others, last_recv.at[s]).wait()

    @pl.loop(0, subsets - 1)
    def _(s):
        arrived(s)
        for k in range(step // 2):
            first = s * step + 2 * k
            y = y_acc[s * (step // 2) + k] + rows_of(n - 1, first)

            def store(i, lines, value):
                image_ref[first + i, lines, :] = value

            second_stage(y, scale, twist_ref, b_hi_ref, b_lo_ref, store)

    for c in range(n):
        if relay and c == RELAY:
            relay_done()
            continue
        sent = stage[c].at[pl.ds(0, rows - piece)]
        pltpu.make_async_copy(sent, sent, part_send.at[c]).wait()
    for u in range(len(units)):
        for i in reach:
            pl.when(p >= i + 1)(lambda u=u, i=i: halo(u, i).wait_send())
    arrived(subsets - 1)


def fused(spec, src, offsets, weights, tables, chunks, counts, step, rng_count, az_count):
    rows, columns = spec.shape[:2]
    blocks = rows // BLOCK
    piece = rows // az_count
    n = len(chunks)
    units = units_of(chunks)
    total_groups = columns // 2 * az_count
    cells = float(rows * rng_count * total_groups * GW) * float(total_groups * GW)
    hbm = pl.BlockSpec(memory_space=pl.ANY)
    tile = (8, GW)
    dma = pltpu.SemaphoreType.DMA
    vmem = pltpu.VMEM
    f32 = jnp.float32
    sizes = [size for _, size in chunks]
    relays = []
    if rng_count == 2 and az_count % 4 == 0 and n - 1 - LAG > RELAY_AT and sizes[RELAY] == 1:
        relays = [vmem((az_count // 4, piece, 1, 1, GW), f32)]
    outs = [
        vmem(((piece - step), 2 * total_groups, GW), f32),
        vmem((piece // 2, 2 * total_groups, 2 * GW), f32),
        vmem((az_count, piece, sizes[-1], 1, GW), f32),
        vmem(tile, f32),
    ] + [vmem(t.shape, t.dtype) for t in tables[n - 1:]]
    return pl.pallas_call(
        functools.partial(fused_kernel, rows, blocks, chunks, units, counts, step, cells),
        out_shape=outs,
        in_specs=[hbm] * (4 + len(tables)),
        out_specs=[pl.BlockSpec(memory_space=vmem)] * len(outs),
        scratch_shapes=[vmem((rows + sum(counts), width, 1, GW), f32) for _, _, width in units]
        + [vmem((rows, size, 1, GW), f32) for size in sizes]
        + [vmem((az_count, piece, size, 1, GW), f32) for size in sizes[:-1]]
        + [vmem(t.shape, t.dtype) for t in tables[:n - 1]]
        + [
            pltpu.SMEM(src.shape, src.dtype),
            vmem(offsets.shape, offsets.dtype),
            vmem(weights.shape, weights.dtype),
            vmem(tile, f32),
            vmem((az_count,) + tile, f32),
            vmem(tile, f32),
            vmem((rng_count,) + tile, f32),
            dma((3,)),
            dma((len(tables),)),
            dma((len(units),)),
            dma((len(units), len(counts))),
            dma((len(units), len(counts))),
            dma((n,)),
            dma((n,)),
            dma((piece // step,)),
            dma((2,)),
            dma((2,)),
            dma((3,)),
        ] + relays,
        compiler_params=pltpu.CompilerParams(
            has_side_effects=True, collective_id=0, vmem_limit_bytes=40 * 1024 * 1024),
    )(src, offsets, weights, spec, *tables)


def store_kernel(step, band_ref, y_acc, recv, scale_ref, a_ref, twist_ref, b_hi_ref, b_lo_ref, out_ref, end, sem, end_sem):
    done = band_ref.shape[0]
    parts = done // step
    az_count, piece, sub = recv.shape[:3]

    def copy(i):
        rows = pl.ds(i * step, step)
        return pltpu.make_async_copy(band_ref.at[rows], out_ref.at[rows], sem.at[i])

    def copy_end(k):
        return pltpu.make_async_copy(end.at[pl.ds(2 * k, 2)], out_ref.at[pl.ds(done + 2 * k, 2)], end_sem.at[k])

    for i in range(parts):
        copy(i).start()

    @pl.loop(0, step // 2)
    def _(k):
        first = done + 2 * k
        y = y_acc[first // 2] + first_stage(recv, a_ref, sub, piece, az_count, first, piece)

        def store(i, lines, value):
            end[2 * k + i, lines, :] = value

        second_stage(y, scale_ref[:1, :1], twist_ref, b_hi_ref, b_lo_ref, store)
        copy_end(k).start()

    for i in range(parts):
        copy(i).wait()
    for k in range(step // 2):
        copy_end(k).wait()


def store(step, rows, band, *rest):
    parts = rows // step
    vmem = pltpu.VMEM
    return pl.pallas_call(
        functools.partial(store_kernel, step),
        out_shape=jax.ShapeDtypeStruct((rows,) + band.shape[1:], band.dtype),
        in_specs=[pl.BlockSpec(memory_space=vmem)] * (1 + len(rest)),
        out_specs=pl.BlockSpec(memory_space=pl.ANY),
        scratch_shapes=[vmem((step,) + band.shape[1:], band.dtype), pltpu.SemaphoreType.DMA((parts - 1,)),
                        pltpu.SemaphoreType.DMA((step // 2,))],
        compiler_params=pltpu.CompilerParams(vmem_limit_bytes=12 * 1024 * 1024),
    )(band, *rest)


def halo_counts(rows_dev, rng_count):
    total = rows_dev * rng_count
    halo = min(rows_dev - BLOCK + SHIFT_B * BLOCK, total - 2 * BLOCK) + WINDOW - rows_dev
    counts = []
    while halo > 0:
        counts.append(min(halo, rows_dev))
        halo -= rows_dev
    return counts


def body(spectrum, src_block, offsets, tap_weights):
    rows_dev = spectrum.shape[0]
    columns = spectrum.shape[2]
    groups = columns // GW
    rng_count = lax.axis_size("rng")
    az_count = lax.axis_size("az")
    rows_after = rows_dev // az_count
    total_len = columns * az_count
    chunks = plan(groups)
    tables = [jnp.asarray(t) for t in dft_tables(az_count, groups, chunks)]
    spec = spectrum.reshape(rows_dev, 2, groups, GW).transpose(0, 2, 1, 3).reshape(rows_dev, 2 * groups, 1, GW)
    counts = halo_counts(rows_dev, rng_count)
    step = min(STEP, rows_after // 2)
    held = fused(spec, src_block.T, offsets, tap_weights, tables, chunks, counts, step, rng_count, az_count)
    image = store(step, rows_after, *held)
    return (
        image.reshape(rows_after, total_len // GW, 2, GW)
        .transpose(0, 2, 1, 3)
        .reshape(rows_after, 2, total_len)
    )


def solution(mesh):
    placed = (P("rng", None, "az"), P("az", "rng"), P("az", "rng"), P(None, "az", "rng"))
    return jax.shard_map(
        body, mesh=mesh, in_specs=placed, out_specs=P(("rng", "az"), None, None), check_vma=False
    )
```

```python
import functools

import jax
import jax.numpy as jnp
import numpy as np
from jax import lax
from jax.experimental import pallas as pl
from jax.experimental.pallas import tpu as pltpu
from jax.sharding import PartitionSpec as P

BLOCK = 128
GW = 128
TAPS = 8
SHIFT_B = 5
WINDOW = 144
UNUSED = WINDOW - (BLOCK - 1 + TAPS)
LAG = 2
RELAY = 7
RELAY_AT = 10
STEP = 4
PAIRS = 4
PAD = 1

MESH = pl.DeviceIdType.MESH


def split_np(x):
    hi = x.astype(jnp.bfloat16)
    lo = (x - hi.astype(np.float64)).astype(jnp.bfloat16)
    return hi, lo


def split(x):
    hi = x.astype(jnp.bfloat16)
    lo = (x - hi.astype(jnp.float32)).astype(jnp.bfloat16)
    return hi, lo


def plan(groups):
    last = max(1, 3 * groups // 16)
    halves = groups // 4
    left = groups - last - halves
    pairs = 2 * left // 9
    sizes = [1] * (2 * halves) + [2] * (left - 2 * pairs) + [4] * pairs + [2 * last]
    starts = [sum(sizes[:i]) for i in range(len(sizes))]
    return tuple(zip(starts, sizes))


def units_of(chunks):
    units = []
    for c, (start, size) in enumerate(chunks):
        width = min(size, 2)
        units += [(c, at, width) for at in range(0, size, width)]
    return tuple(units)


def relays(chunks, rng_count, az_count):
    return rng_count == 2 and az_count % 4 == 0 and len(chunks) - 1 - LAG > RELAY_AT and chunks[RELAY][1] == 1


def gather_sets(chunks, relay):
    sets, held = [[]], 0
    for c, (_, size) in enumerate(chunks[:-1]):
        if relay and c == RELAY:
            continue
        if held + size > 4 and sets[-1]:
            sets.append([])
            held = 0
        sets[-1].append(c)
        held += size
    if relay:
        sets[-1].append(RELAY)
    return tuple(tuple(members) for members in sets) + ((len(chunks) - 1,),)


def dft_tables(az_count, groups, chunks, sets):
    total_groups = az_count * groups
    total_len = total_groups * GW
    k1 = np.arange(total_groups)
    gl, az = np.meshgrid(np.arange(groups), np.arange(az_count), indexing="ij")
    angle = 2.0 * np.pi * ((k1[:, None, None] * (az * groups + gl)[None]) % total_groups) / total_groups
    first = np.empty((2, total_groups, groups, 2, az_count))
    first[0, :, :, 0] = np.cos(angle)
    first[0, :, :, 1] = -np.sin(angle)
    first[1, :, :, 0] = np.sin(angle)
    first[1, :, :, 1] = np.cos(angle)
    first = first.reshape(2 * total_groups, 2 * groups, az_count)
    stage_one = []
    for members in sets:
        columns = [h for c in members for h in range(chunks[c][0], sum(chunks[c]))]
        hi, lo = split_np(first[:, columns].reshape(2 * total_groups, len(columns) * az_count))
        stage_one.append(np.concatenate([hi, hi, lo], axis=1))
    l = np.arange(GW)
    turn = 2.0 * np.pi * (k1[:, None] * l[None, :]) / total_len
    twist = np.stack([np.cos(turn), np.sin(turn)]).astype(np.float32) / np.float32(total_len)
    inner = 2.0 * np.pi * ((l[:, None] * l[None, :]) % GW) / GW
    second = np.empty((2, GW, 2, GW))
    second[0, :, 0] = np.cos(inner)
    second[0, :, 1] = -np.sin(inner)
    second[1, :, 0] = np.sin(inner)
    second[1, :, 1] = np.cos(inner)
    b_hi, b_lo = split_np(second.reshape(2 * GW, 2 * GW))
    return stage_one + [twist, b_hi, b_lo]


def remap_block(ext, width, out, sub, at, b, src, off, weight_row):
    source = [ext[pl.ds(src * (BLOCK * width) + c, WINDOW, stride=width), :] for c in range(width)]
    source = jnp.concatenate(source, axis=1) if width > 1 else source[0]
    where = lax.broadcasted_iota(jnp.int32, (WINDOW, BLOCK), 0) - off
    taps = jnp.zeros((WINDOW, BLOCK), jnp.float32)
    for t in range(TAPS):
        taps = jnp.where(where == t, weight_row(t), taps)
    t_hi, t_lo = split(taps)
    s_hi, s_lo = split(source)
    left = jnp.concatenate([t_hi, t_lo, t_hi], axis=0)
    right = jnp.concatenate([s_hi, s_hi, s_lo], axis=0)
    value = lax.dot_general(
        left, right, (((0,), (0,)), ((), ())), preferred_element_type=jnp.float32
    )
    energy = jnp.zeros((8, GW), jnp.float32)
    for c in range(width):
        half = value[:, c * GW:(c + 1) * GW]
        out[pl.ds(b * BLOCK * sub + at + c, BLOCK, stride=sub), :] = half
        energy = energy + jnp.sum((half * half).reshape(BLOCK // 8, 8, GW), axis=0)
    return energy


def first_stage(parts, a_ref, row):
    columns = []
    for k in range(2):
        lines = []
        for recv in parts:
            az_count, stored, sub = recv.shape[:3]
            flat = recv.reshape(az_count * stored * sub, GW)
            lines += [flat[pl.ds((row + k) * sub + s, az_count, stride=stored * sub), :] for s in range(sub)]
        columns.append(jnp.concatenate(lines, axis=0))
    x_hi, x_lo = split(jnp.concatenate(columns, axis=1))
    return jnp.dot(
        a_ref[...], jnp.concatenate([x_hi, x_lo, x_hi], axis=0), preferred_element_type=jnp.float32)


def second_stage(y, twist_ref, b_hi_ref, b_lo_ref, store):
    total_groups = y.shape[0] // 2
    halves = total_groups // GW
    nt = (((1,), (1,)), ((), ()))
    t_re, t_im = twist_ref[0], twist_ref[1]
    turned = []
    for i in range(2):
        y_re = y[:total_groups, i * GW:(i + 1) * GW]
        y_im = y[total_groups:, i * GW:(i + 1) * GW]
        turned.append(jnp.concatenate([y_re * t_re - y_im * t_im, y_re * t_im + y_im * t_re], axis=1))
    z_hi, z_lo = split(jnp.concatenate(turned, axis=0))
    v = (
        lax.dot_general(b_hi_ref[...], z_hi, nt, preferred_element_type=jnp.float32)
        + lax.dot_general(b_hi_ref[...], z_lo, nt, preferred_element_type=jnp.float32)
        + lax.dot_general(b_lo_ref[...], z_hi, nt, preferred_element_type=jnp.float32)
    )
    for i in range(2):
        for c in range(2):
            for h in range(halves):
                store(i, pl.ds(2 * h + c, GW, stride=2 * halves),
                      v[c * GW:(c + 1) * GW, i * total_groups + h * GW:i * total_groups + (h + 1) * GW])


def fused_kernel(rows, blocks, chunks, sets, units, counts, step, cells, src_hbm, off_hbm, w_hbm, spec_ref, *rest):
    n, m = len(chunks), len(sets)
    tables_hbm, rest = rest[:m + 3], rest[m + 3:]
    image_ref, y_acc, last_recv_ref, scale_ref, a_last, twist_ref, b_hi_ref, b_lo_ref = rest[:8]
    scratch = rest[8:]
    ext, scratch = scratch[:len(units)], scratch[len(units):]
    stage, scratch = scratch[:n], scratch[n:]
    recv, scratch = scratch[:n - 1] + (last_recv_ref,), scratch[n - 1:]
    a_refs, scratch = scratch[:m - 1] + (a_last,), scratch[m - 1:]
    tables = a_refs + (twist_ref, b_hi_ref, b_lo_ref)
    (src_ref, off_ref, w_ref, e_own, e_az, e_sum, e_rng, small_sem, table_sem, local_sem, halo_send, halo_recv,
     part_send, part_recv, last_recv, e_send, e_recv, relay_sem, *relay) = scratch
    rng_count, az_count = lax.axis_size("rng"), lax.axis_size("az")
    p, q = lax.axis_index("rng"), lax.axis_index("az")
    piece = rows // az_count
    half = max(az_count // 2, 1)
    side, place = q // half, q % half
    subsets = piece // step
    reach = [i for i in range(len(counts)) if i + 1 < rng_count]

    barrier = pltpu.get_barrier_semaphore()

    @pl.loop(1, rng_count)
    def _(j):
        pl.semaphore_signal(barrier, inc=1, device_id={"rng": (p + j) % rng_count}, device_id_type=MESH)

    @pl.loop(1, az_count)
    def _(j):
        pl.semaphore_signal(barrier, inc=1, device_id={"az": (q + j) % az_count}, device_id_type=MESH)

    def column(u):
        c, at, width = units[u]
        return pl.ds(chunks[c][0] + at, width)

    def local(u):
        return pltpu.make_async_copy(
            spec_ref.at[:, column(u)], ext[u].at[pl.ds(0, rows)], local_sem.at[u])

    def halo(u, i):
        source = ext[u].at[pl.ds(0, counts[i])] if u == 0 else spec_ref.at[pl.ds(0, counts[i]), column(u)]
        return pltpu.make_async_remote_copy(
            src_ref=source,
            dst_ref=ext[u].at[pl.ds(rows + sum(counts[:i]), counts[i])],
            send_sem=halo_send.at[u, i], recv_sem=halo_recv.at[u, i],
            device_id={"rng": (p + rng_count - i - 1) % rng_count}, device_id_type=MESH)

    def table(i):
        return pltpu.make_async_copy(tables_hbm[i], tables[i], table_sem.at[i])

    local(0).start()
    small = [pltpu.make_async_copy(hbm, ref, small_sem.at[i])
             for i, (hbm, ref) in enumerate(((src_hbm, src_ref), (off_hbm, off_ref), (w_hbm, w_ref)))]
    for copy in small:
        copy.start()
    local(0).wait()
    pl.semaphore_wait(barrier, rng_count + az_count - 2)

    for u in range(len(units)):
        for i in reach:
            pl.when(p >= i + 1)(lambda u=u, i=i: halo(u, i).start())
    for u in range(1, len(units)):
        local(u).start()
    for i in range(m + 3):
        table(i).start()
    for u, (_, _, width) in enumerate(units):
        ext[u][pl.ds(rows + sum(counts), UNUSED)] = jnp.zeros((UNUSED, width, 1, GW), jnp.float32)
    for copy in small:
        copy.wait()

    def arrive(u):
        if u:
            local(u).wait()
        for i in reach:
            pl.when(p + i + 1 < rng_count)(lambda: halo(u, i).wait_recv())

    def remap(u, b):
        c, at, width = units[u]
        g, sub = (chunks[c][0] + at) // 2, chunks[c][1]
        lanes = pl.ds(b * BLOCK if isinstance(b, int) else pl.multiple_of(b * BLOCK, BLOCK), BLOCK)
        return remap_block(
            ext[u].reshape(ext[u].shape[0] * width, GW), width, stage[c].reshape(rows * sub, GW), sub, at, b,
            jnp.maximum(src_ref[b, g] - p * blocks, 0), off_ref[pl.ds(g, 1), lanes],
            lambda t: w_ref[t, pl.ds(g, 1), lanes])

    def keep(c):
        recv[c][q, pl.ds(0, piece)] = stage[c][pl.ds(q * piece, piece)]

    def remap_chunk(c):
        energy = jnp.zeros((8, GW), jnp.float32)
        for u in range(len(units)):
            if units[u][0] == c:
                arrive(u)
                energy = lax.fori_loop(0, blocks, lambda b, e, u=u: e + remap(u, b), energy)
        keep(c)
        return energy

    def spread(send):
        @pl.loop(0, half)
        def _(j):
            send((1 - side) * half + (place + j) % half)

        @pl.loop(1, half)
        def _(j):
            send(side * half + (place + j) % half)

    def send_piece(c, peer):
        pltpu.make_async_remote_copy(
            src_ref=stage[c].at[pl.ds(peer * piece, piece)],
            dst_ref=recv[c].at[q, pl.ds(0, piece)],
            send_sem=part_send.at[c], recv_sem=part_recv.at[c],
            device_id={"az": peer}, device_id_type=MESH).start()

    def hand_over(peer):
        pltpu.make_async_remote_copy(
            src_ref=stage[RELAY].at[pl.ds(peer * piece, piece)],
            dst_ref=relay[0].at[peer % half // 2],
            send_sem=relay_sem.at[0], recv_sem=relay_sem.at[1],
            device_id={"rng": 1 - p}, device_id_type=MESH).start()

    def send_relayed():
        @pl.loop(0, half)
        def _(j):
            peer = (1 - side) * half + (place + j) % half
            via = (p == 0) & (peer % 2 == 0)
            pl.when(via)(lambda: hand_over(peer))
            pl.when(jnp.logical_not(via))(lambda: send_piece(RELAY, peer))

        @pl.loop(1, half)
        def _(j):
            send_piece(RELAY, side * half + (place + j) % half)

    def forward():
        pltpu.make_async_copy(relay[0], relay[0], relay_sem.at[1]).wait()

        @pl.loop(0, half // 2)
        def _(i):
            pltpu.make_async_remote_copy(
                src_ref=relay[0].at[i],
                dst_ref=recv[RELAY].at[q, pl.ds(0, piece)],
                send_sem=relay_sem.at[2], recv_sem=part_recv.at[RELAY],
                device_id={"rng": 1 - p, "az": (1 - side) * half + 2 * i}, device_id_type=MESH).start()

    def relay_done():
        def handed():
            sent = stage[RELAY].at[pl.ds(0, rows - piece - half // 2 * piece)]
            pltpu.make_async_copy(sent, sent, part_send.at[RELAY]).wait()
            pltpu.make_async_copy(relay[0], relay[0], relay_sem.at[0]).wait()

        def forwarded():
            sent = stage[RELAY].at[pl.ds(0, rows - piece)]
            pltpu.make_async_copy(sent, sent, part_send.at[RELAY]).wait()
            pltpu.make_async_copy(relay[0], relay[0], relay_sem.at[2]).wait()

        pl.when(p == 0)(handed)
        pl.when(p != 0)(forwarded)

    def first_chunk():
        peers = BLOCK // piece
        energy = jnp.zeros((8, GW), jnp.float32)
        arrive(0)
        for k in range(blocks):
            b = (k + (1 - side) * (blocks // 2)) % blocks
            energy = energy + remap(0, b)

            @pl.loop(0, peers)
            def _(j):
                peer = b * peers + (place + j) % peers
                pl.when(peer != q)(lambda: send_piece(0, peer))

        keep(0)
        return energy

    def send_last():
        c = n - 1

        @pl.loop(0, subsets)
        def _(r):
            spread(lambda peer: pltpu.make_async_remote_copy(
                src_ref=stage[c].at[pl.ds(peer * piece + r * step, step)],
                dst_ref=recv[c].at[q, pl.ds(r * step, step)],
                send_sem=part_send.at[c], recv_sem=last_recv.at[r],
                device_id={"az": peer}, device_id_type=MESH).start())

    def rows_of(at, row):
        return first_stage([recv[c] for c in sets[at]], a_refs[at], row)

    def gather(at):
        table(at).wait()
        for c in sets[at]:
            others = recv[c].at[pl.ds(0, az_count - 1), pl.ds(0, piece)]
            pltpu.make_async_copy(others, others, part_recv.at[c]).wait()
        pairs = min(PAIRS, piece // 2)

        @pl.loop(0, piece // 2, step=pairs)
        def _(first):
            for k in range(pairs):
                y = rows_of(at, 2 * (first + k))
                y_acc[first + k] = y if at == 0 else y_acc[first + k] + y

    def share(src, dst, slot, axis, peer, at):
        return pltpu.make_async_remote_copy(
            src_ref=src, dst_ref=dst.at[slot], send_sem=e_send.at[at],
            recv_sem=e_recv.at[at], device_id={axis: peer}, device_id_type=MESH)

    def share_all(src, dst, slot, axis, count, at):
        dst[slot] = src[...]

        @pl.loop(1, count)
        def _(j):
            share(src, dst, slot, axis, (slot + j) % count, at).start()

    def share_wait(dst, count, at):
        others = dst.at[pl.ds(0, count - 1)]
        pltpu.make_async_copy(others, others, e_send.at[at]).wait()
        pltpu.make_async_copy(others, others, e_recv.at[at]).wait()

    energy = first_chunk()
    for c in range(1, n - 1):
        energy = energy + remap_chunk(c)
        if relay and c == RELAY:
            send_relayed()
        else:
            spread(functools.partial(send_piece, c))
        for at in range(m - 1):
            if max(sets[at]) == c - LAG:
                gather(at)
        if relay and c == RELAY_AT:
            pl.when(p != 0)(forward)
    energy = energy + remap_chunk(n - 1)
    e_own[...] = energy
    share_all(e_own, e_az, q, "az", az_count, 0)
    send_last()
    for at in range(m - 1):
        if max(sets[at]) > n - 2 - LAG:
            gather(at)
    for i in range(m - 1, m + 3):
        table(i).wait()

    def energy_on():
        share_wait(e_az, az_count, 0)
        e_sum[...] = jnp.sum(e_az[...], axis=0)
        share_all(e_sum, e_rng, p, "rng", rng_count, 1)

    def arrived(s):
        others = recv[n - 1].at[pl.ds(0, az_count - 1), pl.ds(s * step, step)]
        pltpu.make_async_copy(others, others, last_recv.at[s]).wait()

    @pl.loop(0, subsets - 1)
    def _(s):
        pl.when(s == (subsets - 1) // 2)(energy_on)
        arrived(s)
        for k in range(step // 2):
            first = s * step + 2 * k
            y = y_acc[s * (step // 2) + k] + rows_of(m - 1, first)

            def store(i, lines, value):
                image_ref[first + i, lines, :] = value

            second_stage(y, twist_ref, b_hi_ref, b_lo_ref, store)

    for c in range(n):
        if relay and c == RELAY:
            relay_done()
            continue
        sent = stage[c].at[pl.ds(0, rows - piece)]
        pltpu.make_async_copy(sent, sent, part_send.at[c]).wait()
    for u in range(len(units)):
        for i in reach:
            pl.when(p >= i + 1)(lambda u=u, i=i: halo(u, i).wait_send())
    share_wait(e_rng, rng_count, 1)
    mean = jnp.sum(jnp.sum(e_rng[...], axis=0), axis=(0, 1), keepdims=True) / cells
    scale_ref[...] = jnp.broadcast_to(lax.rsqrt(mean + 1e-06), scale_ref.shape)
    arrived(subsets - 1)


def fused(spec, src, offsets, weights, tables, chunks, sets, counts, step, rng_count, az_count):
    rows, columns = spec.shape[:2]
    blocks = rows // BLOCK
    piece = rows // az_count
    m = len(sets)
    units = units_of(chunks)
    total_groups = columns // 2 * az_count
    cells = float(rows * rng_count * total_groups * GW) * float(total_groups * GW)
    hbm = pl.BlockSpec(memory_space=pl.ANY)
    tile = (8, GW)
    dma = pltpu.SemaphoreType.DMA
    vmem = pltpu.VMEM
    f32 = jnp.float32
    sizes = [size for _, size in chunks]
    relay = [vmem((az_count // 4, piece, 1, 1, GW), f32)] if relays(chunks, rng_count, az_count) else []
    outs = [
        vmem(((piece - step), 2 * total_groups, GW), f32),
        vmem((piece // 2, 2 * total_groups, 2 * GW), f32),
        vmem((az_count, piece + PAD, sizes[-1], 1, GW), f32),
        vmem(tile, f32),
    ] + [vmem(t.shape, t.dtype) for t in tables[m - 1:]]
    return pl.pallas_call(
        functools.partial(fused_kernel, rows, blocks, chunks, sets, units, counts, step, cells),
        out_shape=outs,
        in_specs=[hbm] * (4 + len(tables)),
        out_specs=[pl.BlockSpec(memory_space=vmem)] * len(outs),
        scratch_shapes=[vmem((rows + sum(counts) + UNUSED, width, 1, GW), f32) for _, _, width in units]
        + [vmem((rows, size, 1, GW), f32) for size in sizes]
        + [vmem((az_count, piece + PAD, size, 1, GW), f32) for size in sizes[:-1]]
        + [vmem(t.shape, t.dtype) for t in tables[:m - 1]]
        + [
            pltpu.SMEM(src.shape, src.dtype),
            vmem(offsets.shape, offsets.dtype),
            vmem(weights.shape, weights.dtype),
            vmem(tile, f32),
            vmem((az_count,) + tile, f32),
            vmem(tile, f32),
            vmem((rng_count,) + tile, f32),
            dma((3,)),
            dma((len(tables),)),
            dma((len(units),)),
            dma((len(units), len(counts))),
            dma((len(units), len(counts))),
            dma((len(chunks),)),
            dma((len(chunks),)),
            dma((piece // step,)),
            dma((2,)),
            dma((2,)),
            dma((3,)),
        ] + relay,
        compiler_params=pltpu.CompilerParams(
            has_side_effects=True, collective_id=0, vmem_limit_bytes=40 * 1024 * 1024),
    )(src, offsets, weights, spec, *tables)


def store_kernel(step, band_ref, y_acc, recv, scale_ref, a_ref, twist_ref, b_hi_ref, b_lo_ref, out_ref, scaled, sem, end_sem):
    done = band_ref.shape[0]
    scale = scale_ref[:1, :1]

    def copy(first, count, at):
        return pltpu.make_async_copy(scaled.at[pl.ds(first, count)], out_ref.at[pl.ds(first, count)], at)

    @pl.loop(0, done // step)
    def _(i):
        rows = pl.ds(i * step, step)
        scaled[rows] = band_ref[rows] * scale
        copy(i * step, step, sem.at[i]).start()

    @pl.loop(0, step // 2)
    def _(k):
        first = done + 2 * k
        y = y_acc[first // 2] + first_stage([recv], a_ref, first)

        def store(i, lines, value):
            scaled[first + i, lines, :] = value * scale

        second_stage(y, twist_ref, b_hi_ref, b_lo_ref, store)
        copy(first, 2, end_sem.at[k]).start()

    @pl.loop(0, done // step)
    def _(i):
        copy(i * step, step, sem.at[i]).wait()

    @pl.loop(0, step // 2)
    def _(k):
        copy(done + 2 * k, 2, end_sem.at[k]).wait()


def store(step, rows, band, *rest):
    parts = rows // step
    vmem = pltpu.VMEM
    shape = (rows,) + band.shape[1:]
    return pl.pallas_call(
        functools.partial(store_kernel, step),
        out_shape=jax.ShapeDtypeStruct(shape, band.dtype),
        in_specs=[pl.BlockSpec(memory_space=vmem)] * (1 + len(rest)),
        out_specs=pl.BlockSpec(memory_space=pl.ANY),
        scratch_shapes=[vmem(shape, band.dtype), pltpu.SemaphoreType.DMA((parts - 1,)),
                        pltpu.SemaphoreType.DMA((step // 2,))],
        compiler_params=pltpu.CompilerParams(vmem_limit_bytes=20 * 1024 * 1024),
    )(band, *rest)


def halo_counts(rows_dev, rng_count):
    total = rows_dev * rng_count
    halo = min(rows_dev - BLOCK + SHIFT_B * BLOCK, total - 2 * BLOCK) + WINDOW - rows_dev
    counts = []
    while halo > 0:
        counts.append(min(halo, rows_dev) if halo > rows_dev else halo - UNUSED)
        halo -= rows_dev
    return counts


def body(spectrum, src_block, offsets, tap_weights):
    rows_dev = spectrum.shape[0]
    columns = spectrum.shape[2]
    groups = columns // GW
    rng_count = lax.axis_size("rng")
    az_count = lax.axis_size("az")
    rows_after = rows_dev // az_count
    total_len = columns * az_count
    chunks = plan(groups)
    sets = gather_sets(chunks, relays(chunks, rng_count, az_count))
    tables = [jnp.asarray(t) for t in dft_tables(az_count, groups, chunks, sets)]
    spec = spectrum.reshape(rows_dev, 2, groups, GW).transpose(0, 2, 1, 3).reshape(rows_dev, 2 * groups, 1, GW)
    counts = halo_counts(rows_dev, rng_count)
    step = min(STEP, rows_after // 2)
    held = fused(spec, src_block.T, offsets, tap_weights, tables, chunks, sets, counts, step, rng_count, az_count)
    image = store(step, rows_after, *held)
    return (
        image.reshape(rows_after, total_len // GW, 2, GW)
        .transpose(0, 2, 1, 3)
        .reshape(rows_after, 2, total_len)
    )


def solution(mesh):
    placed = (P("rng", None, "az"), P("az", "rng"), P("az", "rng"), P(None, "az", "rng"))
    return jax.shard_map(
        body, mesh=mesh, in_specs=placed, out_specs=P(("rng", "az"), None, None), check_vma=False
    )
```

```python
import functools

import jax
import jax.numpy as jnp
import numpy as np
from jax import lax
from jax.experimental import pallas as pl
from jax.experimental.pallas import tpu as pltpu
from jax.sharding import PartitionSpec as P

BLOCK = 128
GW = 128
TAPS = 8
SHIFT_B = 5
WINDOW = 144
UNUSED = WINDOW - (BLOCK - 1 + TAPS)
LAG = 3
RELAY = 7
RELAY_AT = 10
STEP = 4
PAIRS = 4
PAD = 1

MESH = pl.DeviceIdType.MESH


def split_np(x):
    hi = x.astype(jnp.bfloat16)
    lo = (x - hi.astype(np.float64)).astype(jnp.bfloat16)
    return hi, lo


def split(x):
    hi = x.astype(jnp.bfloat16)
    lo = (x - hi.astype(jnp.float32)).astype(jnp.bfloat16)
    return hi, lo


def plan(groups):
    last = max(1, 3 * groups // 16)
    halves = groups // 4
    left = groups - last - halves
    pairs = 2 * left // 9
    sizes = [1] * (2 * halves) + [2] * (left - 2 * pairs) + [4] * pairs + [2 * last]
    starts = [sum(sizes[:i]) for i in range(len(sizes))]
    return tuple(zip(starts, sizes))


def units_of(chunks):
    units = []
    for c, (start, size) in enumerate(chunks):
        width = min(size, 2)
        units += [(c, at, width) for at in range(0, size, width)]
    return tuple(units)


def relays(chunks, rng_count, az_count):
    return rng_count == 2 and az_count % 4 == 0 and len(chunks) - 1 - LAG > RELAY_AT and chunks[RELAY][1] == 1


def gather_sets(chunks, relay):
    sets, held = [[]], 0
    for c, (_, size) in enumerate(chunks[:-1]):
        if relay and c == RELAY:
            continue
        if held + size > 4 and sets[-1]:
            sets.append([])
            held = 0
        sets[-1].append(c)
        held += size
    if relay:
        sets[-1].append(RELAY)
    return tuple(tuple(members) for members in sets) + ((len(chunks) - 1,),)


def dft_tables(az_count, groups, chunks, sets):
    total_groups = az_count * groups
    total_len = total_groups * GW
    k1 = np.arange(total_groups)
    gl, az = np.meshgrid(np.arange(groups), np.arange(az_count), indexing="ij")
    angle = 2.0 * np.pi * ((k1[:, None, None] * (az * groups + gl)[None]) % total_groups) / total_groups
    first = np.empty((2, total_groups, groups, 2, az_count))
    first[0, :, :, 0] = np.cos(angle)
    first[0, :, :, 1] = -np.sin(angle)
    first[1, :, :, 0] = np.sin(angle)
    first[1, :, :, 1] = np.cos(angle)
    first = first.reshape(2 * total_groups, 2 * groups, az_count)
    stage_one = []
    for members in sets:
        columns = [h for c in members for h in range(chunks[c][0], sum(chunks[c]))]
        hi, lo = split_np(first[:, columns].reshape(2 * total_groups, len(columns) * az_count))
        stage_one.append(np.concatenate([hi, hi, lo], axis=1))
    l = np.arange(GW)
    turn = 2.0 * np.pi * (k1[:, None] * l[None, :]) / total_len
    twist = np.stack([np.cos(turn), np.sin(turn)]).astype(np.float32) / np.float32(total_len)
    inner = 2.0 * np.pi * ((l[:, None] * l[None, :]) % GW) / GW
    second = np.empty((2, GW, 2, GW))
    second[0, :, 0] = np.cos(inner)
    second[0, :, 1] = -np.sin(inner)
    second[1, :, 0] = np.sin(inner)
    second[1, :, 1] = np.cos(inner)
    b_hi, b_lo = split_np(second.reshape(2 * GW, 2 * GW))
    return stage_one + [twist, b_hi, b_lo]


def remap_block(ext, width, out, sub, at, b, src, off, weight_row):
    source = [ext[pl.ds(src * (BLOCK * width) + c, WINDOW, stride=width), :] for c in range(width)]
    source = jnp.concatenate(source, axis=1) if width > 1 else source[0]
    where = lax.broadcasted_iota(jnp.int32, (WINDOW, BLOCK), 0) - off
    taps = jnp.zeros((WINDOW, BLOCK), jnp.float32)
    for t in range(TAPS):
        taps = jnp.where(where == t, weight_row(t), taps)
    t_hi, t_lo = split(taps)
    s_hi, s_lo = split(source)
    left = jnp.concatenate([t_hi, t_lo, t_hi], axis=0)
    right = jnp.concatenate([s_hi, s_hi, s_lo], axis=0)
    value = lax.dot_general(
        left, right, (((0,), (0,)), ((), ())), preferred_element_type=jnp.float32
    )
    energy = jnp.zeros((8, GW), jnp.float32)
    for c in range(width):
        half = value[:, c * GW:(c + 1) * GW]
        out[pl.ds(b * BLOCK * sub + at + c, BLOCK, stride=sub), :] = half
        energy = energy + jnp.sum((half * half).reshape(BLOCK // 8, 8, GW), axis=0)
    return energy


def first_stage(parts, a_ref, row):
    columns = []
    for k in range(2):
        lines = []
        for recv in parts:
            az_count, stored, sub = recv.shape[:3]
            flat = recv.reshape(az_count * stored * sub, GW)
            lines += [flat[pl.ds((row + k) * sub + s, az_count, stride=stored * sub), :] for s in range(sub)]
        columns.append(jnp.concatenate(lines, axis=0))
    x_hi, x_lo = split(jnp.concatenate(columns, axis=1))
    return jnp.dot(
        a_ref[...], jnp.concatenate([x_hi, x_lo, x_hi], axis=0), preferred_element_type=jnp.float32)


def second_stage(y, twist_ref, b_hi_ref, b_lo_ref, store):
    total_groups = y.shape[0] // 2
    halves = total_groups // GW
    nt = (((1,), (1,)), ((), ()))
    t_re, t_im = twist_ref[0], twist_ref[1]
    turned = []
    for i in range(2):
        y_re = y[:total_groups, i * GW:(i + 1) * GW]
        y_im = y[total_groups:, i * GW:(i + 1) * GW]
        turned.append(jnp.concatenate([y_re * t_re - y_im * t_im, y_re * t_im + y_im * t_re], axis=1))
    z_hi, z_lo = split(jnp.concatenate(turned, axis=0))
    v = (
        lax.dot_general(b_hi_ref[...], z_hi, nt, preferred_element_type=jnp.float32)
        + lax.dot_general(b_hi_ref[...], z_lo, nt, preferred_element_type=jnp.float32)
        + lax.dot_general(b_lo_ref[...], z_hi, nt, preferred_element_type=jnp.float32)
    )
    for i in range(2):
        for c in range(2):
            for h in range(halves):
                store(i, pl.ds(2 * h + c, GW, stride=2 * halves),
                      v[c * GW:(c + 1) * GW, i * total_groups + h * GW:i * total_groups + (h + 1) * GW])


def fused_kernel(rows, blocks, chunks, sets, units, counts, step, cells, src_hbm, off_hbm, w_hbm, spec_ref, *rest):
    n, m = len(chunks), len(sets)
    tables_hbm, rest = rest[:m + 3], rest[m + 3:]
    image_ref, y_acc, last_recv_ref, scale_ref, a_last, twist_ref, b_hi_ref, b_lo_ref = rest[:8]
    scratch = rest[8:]
    ext, scratch = scratch[:len(units)], scratch[len(units):]
    stage, scratch = scratch[:n], scratch[n:]
    recv, scratch = scratch[:n - 1] + (last_recv_ref,), scratch[n - 1:]
    a_refs, scratch = scratch[:m - 1] + (a_last,), scratch[m - 1:]
    tables = a_refs + (twist_ref, b_hi_ref, b_lo_ref)
    (src_ref, off_ref, w_ref, e_own, e_az, e_sum, e_rng, small_sem, table_sem, local_sem, halo_send, halo_recv,
     part_send, part_recv, last_recv, e_send, e_recv, relay_sem, *relay) = scratch
    rng_count, az_count = lax.axis_size("rng"), lax.axis_size("az")
    p, q = lax.axis_index("rng"), lax.axis_index("az")
    piece = rows // az_count
    half = max(az_count // 2, 1)
    side, place = q // half, q % half
    subsets = piece // step
    reach = [i for i in range(len(counts)) if i + 1 < rng_count]

    barrier = pltpu.get_barrier_semaphore()

    @pl.loop(1, rng_count)
    def _(j):
        pl.semaphore_signal(barrier, inc=1, device_id={"rng": (p + j) % rng_count}, device_id_type=MESH)

    @pl.loop(1, az_count)
    def _(j):
        pl.semaphore_signal(barrier, inc=1, device_id={"az": (q + j) % az_count}, device_id_type=MESH)

    def column(u):
        c, at, width = units[u]
        return pl.ds(chunks[c][0] + at, width)

    def local(u):
        return pltpu.make_async_copy(
            spec_ref.at[:, column(u)], ext[u].at[pl.ds(0, rows)], local_sem.at[u])

    def halo(u, i):
        source = ext[u].at[pl.ds(0, counts[i])] if u == 0 else spec_ref.at[pl.ds(0, counts[i]), column(u)]
        return pltpu.make_async_remote_copy(
            src_ref=source,
            dst_ref=ext[u].at[pl.ds(rows + sum(counts[:i]), counts[i])],
            send_sem=halo_send.at[u, i], recv_sem=halo_recv.at[u, i],
            device_id={"rng": (p + rng_count - i - 1) % rng_count}, device_id_type=MESH)

    def table(i):
        return pltpu.make_async_copy(tables_hbm[i], tables[i], table_sem.at[i])

    local(0).start()
    small = [pltpu.make_async_copy(hbm, ref, small_sem.at[i])
             for i, (hbm, ref) in enumerate(((src_hbm, src_ref), (off_hbm, off_ref), (w_hbm, w_ref)))]
    for copy in small:
        copy.start()
    local(0).wait()
    pl.semaphore_wait(barrier, rng_count + az_count - 2)

    for u in range(len(units)):
        for i in reach:
            pl.when(p >= i + 1)(lambda u=u, i=i: halo(u, i).start())
    for u in range(1, len(units)):
        local(u).start()
    for i in range(m + 3):
        table(i).start()
    for u, (_, _, width) in enumerate(units):
        ext[u][pl.ds(rows + sum(counts), UNUSED)] = jnp.zeros((UNUSED, width, 1, GW), jnp.float32)
    for copy in small:
        copy.wait()

    def arrive(u):
        if u:
            local(u).wait()
        for i in reach:
            pl.when(p + i + 1 < rng_count)(lambda: halo(u, i).wait_recv())

    def remap(u, b):
        c, at, width = units[u]
        g, sub = (chunks[c][0] + at) // 2, chunks[c][1]
        lanes = pl.ds(b * BLOCK if isinstance(b, int) else pl.multiple_of(b * BLOCK, BLOCK), BLOCK)
        return remap_block(
            ext[u].reshape(ext[u].shape[0] * width, GW), width, stage[c].reshape(rows * sub, GW), sub, at, b,
            jnp.maximum(src_ref[b, g] - p * blocks, 0), off_ref[pl.ds(g, 1), lanes],
            lambda t: w_ref[t, pl.ds(g, 1), lanes])

    def keep(c):
        recv[c][q, pl.ds(0, piece)] = stage[c][pl.ds(q * piece, piece)]

    def remap_chunk(c):
        energy = jnp.zeros((8, GW), jnp.float32)
        for u in range(len(units)):
            if units[u][0] == c:
                arrive(u)
                energy = lax.fori_loop(0, blocks, lambda b, e, u=u: e + remap(u, b), energy)
        keep(c)
        return energy

    def spread(send):
        @pl.loop(0, half)
        def _(j):
            send((1 - side) * half + (place + j) % half)

        @pl.loop(1, half)
        def _(j):
            send(side * half + (place + j) % half)

    def send_piece(c, peer):
        pltpu.make_async_remote_copy(
            src_ref=stage[c].at[pl.ds(peer * piece, piece)],
            dst_ref=recv[c].at[q, pl.ds(0, piece)],
            send_sem=part_send.at[c], recv_sem=part_recv.at[c],
            device_id={"az": peer}, device_id_type=MESH).start()

    def hand_over(peer):
        pltpu.make_async_remote_copy(
            src_ref=stage[RELAY].at[pl.ds(peer * piece, piece)],
            dst_ref=relay[0].at[peer % half // 2],
            send_sem=relay_sem.at[0], recv_sem=relay_sem.at[1],
            device_id={"rng": 1 - p}, device_id_type=MESH).start()

    def send_relayed():
        @pl.loop(0, half)
        def _(j):
            peer = (1 - side) * half + (place + j) % half
            via = (p == 0) & (peer % 2 == 0)
            pl.when(via)(lambda: hand_over(peer))
            pl.when(jnp.logical_not(via))(lambda: send_piece(RELAY, peer))

        @pl.loop(1, half)
        def _(j):
            send_piece(RELAY, side * half + (place + j) % half)

    def forward():
        pltpu.make_async_copy(relay[0], relay[0], relay_sem.at[1]).wait()

        @pl.loop(0, half // 2)
        def _(i):
            pltpu.make_async_remote_copy(
                src_ref=relay[0].at[i],
                dst_ref=recv[RELAY].at[q, pl.ds(0, piece)],
                send_sem=relay_sem.at[2], recv_sem=part_recv.at[RELAY],
                device_id={"rng": 1 - p, "az": (1 - side) * half + 2 * i}, device_id_type=MESH).start()

    def relay_done():
        def handed():
            sent = stage[RELAY].at[pl.ds(0, rows - piece - half // 2 * piece)]
            pltpu.make_async_copy(sent, sent, part_send.at[RELAY]).wait()
            pltpu.make_async_copy(relay[0], relay[0], relay_sem.at[0]).wait()

        def forwarded():
            sent = stage[RELAY].at[pl.ds(0, rows - piece)]
            pltpu.make_async_copy(sent, sent, part_send.at[RELAY]).wait()
            pltpu.make_async_copy(relay[0], relay[0], relay_sem.at[2]).wait()

        pl.when(p == 0)(handed)
        pl.when(p != 0)(forwarded)

    def first_chunk():
        peers = BLOCK // piece
        energy = jnp.zeros((8, GW), jnp.float32)
        arrive(0)
        for k in range(blocks):
            b = (k + (1 - side) * (blocks // 2)) % blocks
            energy = energy + remap(0, b)

            @pl.loop(0, peers)
            def _(j):
                peer = b * peers + (place + j) % peers
                pl.when(peer != q)(lambda: send_piece(0, peer))

        keep(0)
        return energy

    def send_rows(r, peer):
        c = n - 1
        pltpu.make_async_remote_copy(
            src_ref=stage[c].at[pl.ds(peer * piece + r * step, step)],
            dst_ref=recv[c].at[q, pl.ds(r * step, step)],
            send_sem=part_send.at[c], recv_sem=last_recv.at[r],
            device_id={"az": peer}, device_id_type=MESH).start()

    def send_last():
        @pl.loop(0, subsets - 2)
        def _(r):
            spread(functools.partial(send_rows, r))

        quarter = max(half // 2, 1)
        turn = jnp.where(side == 0, place // quarter, 0)

        @pl.loop(0, half // quarter)
        def _(h):
            @pl.loop(subsets - 2, subsets)
            def _(r):
                @pl.loop(0, quarter)
                def _(j):
                    send_rows(r, (1 - side) * half + (h + turn) % (half // quarter) * quarter + (place + j) % quarter)

        @pl.loop(subsets - 2, subsets)
        def _(r):
            @pl.loop(1, half)
            def _(j):
                send_rows(r, side * half + (place + j) % half)

    def rows_of(at, row):
        return first_stage([recv[c] for c in sets[at]], a_refs[at], row)

    def gather(at):
        table(at).wait()
        for c in sets[at]:
            others = recv[c].at[pl.ds(0, az_count - 1), pl.ds(0, piece)]
            pltpu.make_async_copy(others, others, part_recv.at[c]).wait()
        pairs = min(PAIRS, piece // 2)

        @pl.loop(0, piece // 2, step=pairs)
        def _(first):
            for k in range(pairs):
                y = rows_of(at, 2 * (first + k))
                y_acc[first + k] = y if at == 0 else y_acc[first + k] + y

    def share(src, dst, slot, axis, peer, at):
        return pltpu.make_async_remote_copy(
            src_ref=src, dst_ref=dst.at[slot], send_sem=e_send.at[at],
            recv_sem=e_recv.at[at], device_id={axis: peer}, device_id_type=MESH)

    def share_all(src, dst, slot, axis, count, at):
        dst[slot] = src[...]

        @pl.loop(1, count)
        def _(j):
            share(src, dst, slot, axis, (slot + j) % count, at).start()

    def share_wait(dst, count, at):
        others = dst.at[pl.ds(0, count - 1)]
        pltpu.make_async_copy(others, others, e_send.at[at]).wait()
        pltpu.make_async_copy(others, others, e_recv.at[at]).wait()

    energy = first_chunk()
    for c in range(1, n - 1):
        energy = energy + remap_chunk(c)
        if relay and c == RELAY:
            send_relayed()
        else:
            spread(functools.partial(send_piece, c))
        for at in range(m - 1):
            if max(sets[at]) == c - LAG:
                gather(at)
        if relay and c == RELAY_AT:
            pl.when(p != 0)(forward)
    energy = energy + remap_chunk(n - 1)
    e_own[...] = energy
    share_all(e_own, e_az, q, "az", az_count, 0)
    send_last()
    for at in range(m - 1):
        if max(sets[at]) > n - 2 - LAG:
            gather(at)
    for i in range(m - 1, m + 3):
        table(i).wait()

    def energy_on():
        share_wait(e_az, az_count, 0)
        e_sum[...] = jnp.sum(e_az[...], axis=0)
        share_all(e_sum, e_rng, p, "rng", rng_count, 1)

    def arrived(s):
        others = recv[n - 1].at[pl.ds(0, az_count - 1), pl.ds(s * step, step)]
        pltpu.make_async_copy(others, others, last_recv.at[s]).wait()

    @pl.loop(0, subsets - 1)
    def _(s):
        pl.when(s == (subsets - 1) // 2)(energy_on)
        arrived(s)
        for k in range(step // 2):
            first = s * step + 2 * k
            y = y_acc[s * (step // 2) + k] + rows_of(m - 1, first)

            def store(i, lines, value):
                image_ref[first + i, lines, :] = value

            second_stage(y, twist_ref, b_hi_ref, b_lo_ref, store)

    for c in range(n):
        if relay and c == RELAY:
            relay_done()
            continue
        sent = stage[c].at[pl.ds(0, rows - piece)]
        pltpu.make_async_copy(sent, sent, part_send.at[c]).wait()
    for u in range(len(units)):
        for i in reach:
            pl.when(p >= i + 1)(lambda u=u, i=i: halo(u, i).wait_send())
    share_wait(e_rng, rng_count, 1)
    mean = jnp.sum(jnp.sum(e_rng[...], axis=0), axis=(0, 1), keepdims=True) / cells
    scale_ref[...] = jnp.broadcast_to(lax.rsqrt(mean + 1e-06), scale_ref.shape)
    arrived(subsets - 1)


def fused(spec, src, offsets, weights, tables, chunks, sets, counts, step, rng_count, az_count):
    rows, columns = spec.shape[:2]
    blocks = rows // BLOCK
    piece = rows // az_count
    m = len(sets)
    units = units_of(chunks)
    total_groups = columns // 2 * az_count
    cells = float(rows * rng_count * total_groups * GW) * float(total_groups * GW)
    hbm = pl.BlockSpec(memory_space=pl.ANY)
    tile = (8, GW)
    dma = pltpu.SemaphoreType.DMA
    vmem = pltpu.VMEM
    f32 = jnp.float32
    sizes = [size for _, size in chunks]
    relay = [vmem((az_count // 4, piece, 1, 1, GW), f32)] if relays(chunks, rng_count, az_count) else []
    outs = [
        vmem(((piece - step), 2 * total_groups, GW), f32),
        vmem((piece // 2, 2 * total_groups, 2 * GW), f32),
        vmem((az_count, piece + PAD, sizes[-1], 1, GW), f32),
        vmem(tile, f32),
    ] + [vmem(t.shape, t.dtype) for t in tables[m - 1:]]
    return pl.pallas_call(
        functools.partial(fused_kernel, rows, blocks, chunks, sets, units, counts, step, cells),
        out_shape=outs,
        in_specs=[hbm] * (4 + len(tables)),
        out_specs=[pl.BlockSpec(memory_space=vmem)] * len(outs),
        scratch_shapes=[vmem((rows + sum(counts) + UNUSED, width, 1, GW), f32) for _, _, width in units]
        + [vmem((rows, size, 1, GW), f32) for size in sizes]
        + [vmem((az_count, piece + PAD, size, 1, GW), f32) for size in sizes[:-1]]
        + [vmem(t.shape, t.dtype) for t in tables[:m - 1]]
        + [
            pltpu.SMEM(src.shape, src.dtype),
            vmem(offsets.shape, offsets.dtype),
            vmem(weights.shape, weights.dtype),
            vmem(tile, f32),
            vmem((az_count,) + tile, f32),
            vmem(tile, f32),
            vmem((rng_count,) + tile, f32),
            dma((3,)),
            dma((len(tables),)),
            dma((len(units),)),
            dma((len(units), len(counts))),
            dma((len(units), len(counts))),
            dma((len(chunks),)),
            dma((len(chunks),)),
            dma((piece // step,)),
            dma((2,)),
            dma((2,)),
            dma((3,)),
        ] + relay,
        compiler_params=pltpu.CompilerParams(
            has_side_effects=True, collective_id=0, vmem_limit_bytes=40 * 1024 * 1024),
    )(src, offsets, weights, spec, *tables)


def store_kernel(step, band_ref, y_acc, recv, scale_ref, a_ref, twist_ref, b_hi_ref, b_lo_ref, out_ref, scaled, sem, end_sem):
    done = band_ref.shape[0]
    scale = scale_ref[:1, :1]

    def copy(first, count, at):
        return pltpu.make_async_copy(scaled.at[pl.ds(first, count)], out_ref.at[pl.ds(first, count)], at)

    @pl.loop(0, done // step)
    def _(i):
        rows = pl.ds(i * step, step)
        scaled[rows] = band_ref[rows] * scale
        copy(i * step, step, sem.at[i]).start()

    @pl.loop(0, step // 2)
    def _(k):
        first = done + 2 * k
        y = y_acc[first // 2] + first_stage([recv], a_ref, first)

        def store(i, lines, value):
            scaled[first + i, lines, :] = value * scale

        second_stage(y, twist_ref, b_hi_ref, b_lo_ref, store)
        copy(first, 2, end_sem.at[k]).start()

    @pl.loop(0, done // step)
    def _(i):
        copy(i * step, step, sem.at[i]).wait()

    @pl.loop(0, step // 2)
    def _(k):
        copy(done + 2 * k, 2, end_sem.at[k]).wait()


def store(step, rows, band, *rest):
    parts = rows // step
    vmem = pltpu.VMEM
    shape = (rows,) + band.shape[1:]
    return pl.pallas_call(
        functools.partial(store_kernel, step),
        out_shape=jax.ShapeDtypeStruct(shape, band.dtype),
        in_specs=[pl.BlockSpec(memory_space=vmem)] * (1 + len(rest)),
        out_specs=pl.BlockSpec(memory_space=pl.ANY),
        scratch_shapes=[vmem(shape, band.dtype), pltpu.SemaphoreType.DMA((parts - 1,)),
                        pltpu.SemaphoreType.DMA((step // 2,))],
        compiler_params=pltpu.CompilerParams(vmem_limit_bytes=20 * 1024 * 1024),
    )(band, *rest)


def halo_counts(rows_dev, rng_count):
    total = rows_dev * rng_count
    halo = min(rows_dev - BLOCK + SHIFT_B * BLOCK, total - 2 * BLOCK) + WINDOW - rows_dev
    counts = []
    while halo > 0:
        counts.append(min(halo, rows_dev) if halo > rows_dev else halo - UNUSED)
        halo -= rows_dev
    return counts


def body(spectrum, src_block, offsets, tap_weights):
    rows_dev = spectrum.shape[0]
    columns = spectrum.shape[2]
    groups = columns // GW
    rng_count = lax.axis_size("rng")
    az_count = lax.axis_size("az")
    rows_after = rows_dev // az_count
    total_len = columns * az_count
    chunks = plan(groups)
    sets = gather_sets(chunks, relays(chunks, rng_count, az_count))
    tables = [jnp.asarray(t) for t in dft_tables(az_count, groups, chunks, sets)]
    spec = spectrum.reshape(rows_dev, 2, groups, GW).transpose(0, 2, 1, 3).reshape(rows_dev, 2 * groups, 1, GW)
    counts = halo_counts(rows_dev, rng_count)
    step = min(STEP, rows_after // 2)
    held = fused(spec, src_block.T, offsets, tap_weights, tables, chunks, sets, counts, step, rng_count, az_count)
    image = store(step, rows_after, *held)
    return (
        image.reshape(rows_after, total_len // GW, 2, GW)
        .transpose(0, 2, 1, 3)
        .reshape(rows_after, 2, total_len)
    )


def solution(mesh):
    placed = (P("rng", None, "az"), P("az", "rng"), P("az", "rng"), P(None, "az", "rng"))
    return jax.shard_map(
        body, mesh=mesh, in_specs=placed, out_specs=P(("rng", "az"), None, None), check_vma=False
    )
```

```python
import functools

import jax
import jax.numpy as jnp
import numpy as np
from jax import lax
from jax.experimental import pallas as pl
from jax.experimental.pallas import tpu as pltpu
from jax.sharding import PartitionSpec as P

BLOCK = 128
GW = 128
TAPS = 8
SHIFT_B = 5
WINDOW = 144
UNUSED = WINDOW - (BLOCK - 1 + TAPS)
LAG = 3
RELAY = 7
RELAY_AT = 10
STEP = 4
PAIRS = 4
PAD = 1

MESH = pl.DeviceIdType.MESH


def split_np(x):
    hi = x.astype(jnp.bfloat16)
    lo = (x - hi.astype(np.float64)).astype(jnp.bfloat16)
    return hi, lo


def split(x):
    hi = x.astype(jnp.bfloat16)
    lo = (x - hi.astype(jnp.float32)).astype(jnp.bfloat16)
    return hi, lo


def plan(groups):
    last = max(1, 3 * groups // 16)
    halves = groups // 4
    left = groups - last - halves
    pairs = 2 * left // 9
    sizes = [1] * (2 * halves) + [2] * (left - 2 * pairs) + [4] * pairs + [2 * last]
    starts = [sum(sizes[:i]) for i in range(len(sizes))]
    return tuple(zip(starts, sizes))


def units_of(chunks):
    units = []
    for c, (start, size) in enumerate(chunks):
        width = min(size, 2)
        units += [(c, at, width) for at in range(0, size, width)]
    return tuple(units)


def relays(chunks, rng_count, az_count):
    return rng_count == 2 and az_count % 4 == 0 and len(chunks) - 1 - LAG > RELAY_AT and chunks[RELAY][1] == 1


def gather_sets(chunks, relay):
    sets, held = [[]], 0
    for c, (_, size) in enumerate(chunks[:-1]):
        if relay and c == RELAY:
            continue
        if held + size > 4 and sets[-1]:
            sets.append([])
            held = 0
        sets[-1].append(c)
        held += size
    if relay:
        sets[-1].append(RELAY)
    return tuple(tuple(members) for members in sets) + ((len(chunks) - 1,),)


def dft_tables(az_count, groups, chunks, sets):
    total_groups = az_count * groups
    total_len = total_groups * GW
    k1 = np.arange(total_groups)
    gl, az = np.meshgrid(np.arange(groups), np.arange(az_count), indexing="ij")
    angle = 2.0 * np.pi * ((k1[:, None, None] * (az * groups + gl)[None]) % total_groups) / total_groups
    first = np.empty((2, total_groups, groups, 2, az_count))
    first[0, :, :, 0] = np.cos(angle)
    first[0, :, :, 1] = -np.sin(angle)
    first[1, :, :, 0] = np.sin(angle)
    first[1, :, :, 1] = np.cos(angle)
    first = first.reshape(2 * total_groups, 2 * groups, az_count)
    stage_one = []
    for members in sets:
        columns = [h for c in members for h in range(chunks[c][0], sum(chunks[c]))]
        hi, lo = split_np(first[:, columns].reshape(2 * total_groups, len(columns) * az_count))
        stage_one.append(np.concatenate([hi, hi, lo], axis=1))
    l = np.arange(GW)
    turn = 2.0 * np.pi * (k1[:, None] * l[None, :]) / total_len
    twist = np.stack([np.cos(turn), np.sin(turn)]).astype(np.float32) / np.float32(total_len)
    inner = 2.0 * np.pi * ((l[:, None] * l[None, :]) % GW) / GW
    second = np.empty((2, GW, 2, GW))
    second[0, :, 0] = np.cos(inner)
    second[0, :, 1] = -np.sin(inner)
    second[1, :, 0] = np.sin(inner)
    second[1, :, 1] = np.cos(inner)
    b_hi, b_lo = split_np(second.reshape(2 * GW, 2 * GW))
    return stage_one + [twist, b_hi, b_lo]


def remap_block(ext, width, out, sub, at, b, src, off, weight_row):
    source = [ext[pl.ds(src * (BLOCK * width) + c, WINDOW, stride=width), :] for c in range(width)]
    source = jnp.concatenate(source, axis=1) if width > 1 else source[0]
    where = lax.broadcasted_iota(jnp.int32, (WINDOW, BLOCK), 0) - off
    taps = jnp.zeros((WINDOW, BLOCK), jnp.float32)
    for t in range(TAPS):
        taps = jnp.where(where == t, weight_row(t), taps)
    t_hi, t_lo = split(taps)
    s_hi, s_lo = split(source)
    left = jnp.concatenate([t_hi, t_lo, t_hi], axis=0)
    right = jnp.concatenate([s_hi, s_hi, s_lo], axis=0)
    value = lax.dot_general(
        left, right, (((0,), (0,)), ((), ())), preferred_element_type=jnp.float32
    )
    energy = jnp.zeros((8, GW), jnp.float32)
    for c in range(width):
        half = value[:, c * GW:(c + 1) * GW]
        out[pl.ds(b * BLOCK * sub + at + c, BLOCK, stride=sub), :] = half
        energy = energy + jnp.sum((half * half).reshape(BLOCK // 8, 8, GW), axis=0)
    return energy


def first_stage(parts, a_ref, row):
    columns = []
    for k in range(2):
        lines = []
        for recv in parts:
            az_count, stored, sub = recv.shape[:3]
            flat = recv.reshape(az_count * stored * sub, GW)
            lines += [flat[pl.ds((row + k) * sub + s, az_count, stride=stored * sub), :] for s in range(sub)]
        columns.append(jnp.concatenate(lines, axis=0))
    x_hi, x_lo = split(jnp.concatenate(columns, axis=1))
    return jnp.dot(
        a_ref[...], jnp.concatenate([x_hi, x_lo, x_hi], axis=0), preferred_element_type=jnp.float32)


def second_stage(y, twist_ref, b_hi_ref, b_lo_ref, store):
    total_groups = y.shape[0] // 2
    halves = total_groups // GW
    nt = (((1,), (1,)), ((), ()))
    t_re, t_im = twist_ref[0], twist_ref[1]
    turned = []
    for i in range(2):
        y_re = y[:total_groups, i * GW:(i + 1) * GW]
        y_im = y[total_groups:, i * GW:(i + 1) * GW]
        turned.append(jnp.concatenate([y_re * t_re - y_im * t_im, y_re * t_im + y_im * t_re], axis=1))
    z_hi, z_lo = split(jnp.concatenate(turned, axis=0))
    v = (
        lax.dot_general(b_hi_ref[...], z_hi, nt, preferred_element_type=jnp.float32)
        + lax.dot_general(b_hi_ref[...], z_lo, nt, preferred_element_type=jnp.float32)
        + lax.dot_general(b_lo_ref[...], z_hi, nt, preferred_element_type=jnp.float32)
    )
    for i in range(2):
        for c in range(2):
            for h in range(halves):
                store(i, pl.ds(2 * h + c, GW, stride=2 * halves),
                      v[c * GW:(c + 1) * GW, i * total_groups + h * GW:i * total_groups + (h + 1) * GW])


def fused_kernel(rows, blocks, chunks, sets, units, counts, step, cells, src_hbm, off_hbm, w_hbm, spec_ref, *rest):
    n, m = len(chunks), len(sets)
    tables_hbm, rest = rest[:m + 3], rest[m + 3:]
    image_ref, y_acc, last_recv_ref, scale_ref, a_last, twist_ref, b_hi_ref, b_lo_ref = rest[:8]
    scratch = rest[8:]
    ext, scratch = scratch[:len(units)], scratch[len(units):]
    stage, scratch = scratch[:n], scratch[n:]
    recv, scratch = scratch[:n - 1] + (last_recv_ref,), scratch[n - 1:]
    a_refs, scratch = scratch[:m - 1] + (a_last,), scratch[m - 1:]
    tables = a_refs + (twist_ref, b_hi_ref, b_lo_ref)
    (src_ref, off_ref, w_ref, e_own, e_az, e_sum, e_rng, small_sem, table_sem, local_sem, halo_send, halo_recv,
     part_send, part_recv, last_recv, e_send, e_recv, relay_sem, *relay) = scratch
    rng_count, az_count = lax.axis_size("rng"), lax.axis_size("az")
    p, q = lax.axis_index("rng"), lax.axis_index("az")
    piece = rows // az_count
    half = max(az_count // 2, 1)
    side, place = q // half, q % half
    subsets = piece // step
    reach = [i for i in range(len(counts)) if i + 1 < rng_count]

    barrier = pltpu.get_barrier_semaphore()

    @pl.loop(1, rng_count)
    def _(j):
        pl.semaphore_signal(barrier, inc=1, device_id={"rng": (p + j) % rng_count}, device_id_type=MESH)

    @pl.loop(1, az_count)
    def _(j):
        pl.semaphore_signal(barrier, inc=1, device_id={"az": (q + j) % az_count}, device_id_type=MESH)

    def column(u):
        c, at, width = units[u]
        return pl.ds(chunks[c][0] + at, width)

    def local(u):
        return pltpu.make_async_copy(
            spec_ref.at[:, column(u)], ext[u].at[pl.ds(0, rows)], local_sem.at[u])

    def halo(u, i):
        source = ext[u].at[pl.ds(0, counts[i])] if u == 0 else spec_ref.at[pl.ds(0, counts[i]), column(u)]
        return pltpu.make_async_remote_copy(
            src_ref=source,
            dst_ref=ext[u].at[pl.ds(rows + sum(counts[:i]), counts[i])],
            send_sem=halo_send.at[u, i], recv_sem=halo_recv.at[u, i],
            device_id={"rng": (p + rng_count - i - 1) % rng_count}, device_id_type=MESH)

    def table(i):
        return pltpu.make_async_copy(tables_hbm[i], tables[i], table_sem.at[i])

    local(0).start()
    small = [pltpu.make_async_copy(hbm, ref, small_sem.at[i])
             for i, (hbm, ref) in enumerate(((src_hbm, src_ref), (off_hbm, off_ref), (w_hbm, w_ref)))]
    for copy in small:
        copy.start()
    local(0).wait()
    pl.semaphore_wait(barrier, rng_count + az_count - 2)

    for u in range(len(units)):
        for i in reach:
            pl.when(p >= i + 1)(lambda u=u, i=i: halo(u, i).start())
    for u in range(1, len(units)):
        local(u).start()
    for i in range(m + 3):
        table(i).start()
    for u, (_, _, width) in enumerate(units):
        ext[u][pl.ds(rows + sum(counts), UNUSED)] = jnp.zeros((UNUSED, width, 1, GW), jnp.float32)
    for copy in small:
        copy.wait()

    def arrive(u):
        if u:
            local(u).wait()
        for i in reach:
            pl.when(p + i + 1 < rng_count)(lambda: halo(u, i).wait_recv())

    def remap(u, b):
        c, at, width = units[u]
        g, sub = (chunks[c][0] + at) // 2, chunks[c][1]
        lanes = pl.ds(b * BLOCK if isinstance(b, int) else pl.multiple_of(b * BLOCK, BLOCK), BLOCK)
        return remap_block(
            ext[u].reshape(ext[u].shape[0] * width, GW), width, stage[c].reshape(rows * sub, GW), sub, at, b,
            jnp.maximum(src_ref[b, g] - p * blocks, 0), off_ref[pl.ds(g, 1), lanes],
            lambda t: w_ref[t, pl.ds(g, 1), lanes])

    def keep(c):
        recv[c][q, pl.ds(0, piece)] = stage[c][pl.ds(q * piece, piece)]

    def remap_chunk(c):
        energy = jnp.zeros((8, GW), jnp.float32)
        for u in range(len(units)):
            if units[u][0] == c:
                arrive(u)
                energy = lax.fori_loop(0, blocks, lambda b, e, u=u: e + remap(u, b), energy)
        keep(c)
        return energy

    def spread(send):
        @pl.loop(0, half)
        def _(j):
            send((1 - side) * half + (place + j) % half)

        @pl.loop(1, half)
        def _(j):
            send(side * half + (place + j) % half)

    def send_piece(c, peer):
        pltpu.make_async_remote_copy(
            src_ref=stage[c].at[pl.ds(peer * piece, piece)],
            dst_ref=recv[c].at[q, pl.ds(0, piece)],
            send_sem=part_send.at[c], recv_sem=part_recv.at[c],
            device_id={"az": peer}, device_id_type=MESH).start()

    def hand_over(peer):
        pltpu.make_async_remote_copy(
            src_ref=stage[RELAY].at[pl.ds(peer * piece, piece)],
            dst_ref=relay[0].at[peer % half],
            send_sem=relay_sem.at[0], recv_sem=relay_sem.at[1],
            device_id={"rng": 1 - p}, device_id_type=MESH).start()

    def send_relayed():
        @pl.loop(0, half)
        def _(j):
            peer = (1 - side) * half + (place + j) % half
            slot = peer % half
            via = (p == 0) & ((slot < half // 2) | (slot == half - 1))
            pl.when(via)(lambda: hand_over(peer))
            pl.when(jnp.logical_not(via))(lambda: send_piece(RELAY, peer))

        @pl.loop(1, half)
        def _(j):
            send_piece(RELAY, side * half + (place + j) % half)

    def forward():
        sent = relay[0].at[pl.ds(0, (half // 2 + 1))]
        pltpu.make_async_copy(sent, sent, relay_sem.at[1]).wait()

        @pl.loop(0, half)
        def _(slot):
            copy = pltpu.make_async_remote_copy(
                src_ref=relay[0].at[slot],
                dst_ref=recv[RELAY].at[q, pl.ds(0, piece)],
                send_sem=relay_sem.at[2], recv_sem=part_recv.at[RELAY],
                device_id={"rng": 1 - p, "az": (1 - side) * half + slot}, device_id_type=MESH)
            pl.when((slot < half // 2) | (slot == half - 1))(copy.start)

    def relay_done():
        def handed():
            sent = stage[RELAY].at[pl.ds(0, rows - piece - (half // 2 + 1) * piece)]
            pltpu.make_async_copy(sent, sent, part_send.at[RELAY]).wait()
            via = relay[0].at[pl.ds(0, (half // 2 + 1))]
            pltpu.make_async_copy(via, via, relay_sem.at[0]).wait()

        def forwarded():
            sent = stage[RELAY].at[pl.ds(0, rows - piece)]
            pltpu.make_async_copy(sent, sent, part_send.at[RELAY]).wait()
            via = relay[0].at[pl.ds(0, (half // 2 + 1))]
            pltpu.make_async_copy(via, via, relay_sem.at[2]).wait()

        pl.when(p == 0)(handed)
        pl.when(p != 0)(forwarded)

    def first_chunk():
        peers = BLOCK // piece
        energy = jnp.zeros((8, GW), jnp.float32)
        arrive(0)
        for k in range(blocks):
            b = (k + (1 - side) * (blocks // 2)) % blocks
            energy = energy + remap(0, b)

            @pl.loop(0, peers)
            def _(j):
                peer = b * peers + (place + j) % peers
                pl.when(peer != q)(lambda: send_piece(0, peer))

        keep(0)
        return energy

    def send_rows(r, peer):
        c = n - 1
        pltpu.make_async_remote_copy(
            src_ref=stage[c].at[pl.ds(peer * piece + r * step, step)],
            dst_ref=recv[c].at[q, pl.ds(r * step, step)],
            send_sem=part_send.at[c], recv_sem=last_recv.at[r],
            device_id={"az": peer}, device_id_type=MESH).start()

    def send_last():
        @pl.loop(0, subsets - 2)
        def _(r):
            spread(functools.partial(send_rows, r))

        quarter = max(half // 2, 1)
        turn = jnp.where(side == 0, place // quarter, 0)

        @pl.loop(0, half // quarter)
        def _(h):
            @pl.loop(subsets - 2, subsets)
            def _(r):
                @pl.loop(0, quarter)
                def _(j):
                    send_rows(r, (1 - side) * half + (h + turn) % (half // quarter) * quarter + (place + j) % quarter)

        @pl.loop(subsets - 2, subsets)
        def _(r):
            @pl.loop(1, half)
            def _(j):
                send_rows(r, side * half + (place + j) % half)

    def rows_of(at, row):
        return first_stage([recv[c] for c in sets[at]], a_refs[at], row)

    def gather(at):
        table(at).wait()
        for c in sets[at]:
            others = recv[c].at[pl.ds(0, az_count - 1), pl.ds(0, piece)]
            pltpu.make_async_copy(others, others, part_recv.at[c]).wait()
        pairs = min(PAIRS, piece // 2)

        @pl.loop(0, piece // 2, step=pairs)
        def _(first):
            for k in range(pairs):
                y = rows_of(at, 2 * (first + k))
                y_acc[first + k] = y if at == 0 else y_acc[first + k] + y

    def share(src, dst, slot, axis, peer, at):
        return pltpu.make_async_remote_copy(
            src_ref=src, dst_ref=dst.at[slot], send_sem=e_send.at[at],
            recv_sem=e_recv.at[at], device_id={axis: peer}, device_id_type=MESH)

    def share_all(src, dst, slot, axis, count, at):
        dst[slot] = src[...]

        @pl.loop(1, count)
        def _(j):
            share(src, dst, slot, axis, (slot + j) % count, at).start()

    def share_wait(dst, count, at):
        others = dst.at[pl.ds(0, count - 1)]
        pltpu.make_async_copy(others, others, e_send.at[at]).wait()
        pltpu.make_async_copy(others, others, e_recv.at[at]).wait()

    energy = first_chunk()
    for c in range(1, n - 1):
        energy = energy + remap_chunk(c)
        if relay and c == RELAY:
            send_relayed()
        else:
            spread(functools.partial(send_piece, c))
        for at in range(m - 1):
            if max(sets[at]) == c - LAG:
                gather(at)
        if relay and c == RELAY_AT:
            pl.when(p != 0)(forward)
    energy = energy + remap_chunk(n - 1)
    e_own[...] = energy
    share_all(e_own, e_az, q, "az", az_count, 0)
    send_last()
    for at in range(m - 1):
        if max(sets[at]) > n - 2 - LAG:
            gather(at)
    for i in range(m - 1, m + 3):
        table(i).wait()

    def energy_on():
        share_wait(e_az, az_count, 0)
        e_sum[...] = jnp.sum(e_az[...], axis=0)
        share_all(e_sum, e_rng, p, "rng", rng_count, 1)

    def arrived(s):
        others = recv[n - 1].at[pl.ds(0, az_count - 1), pl.ds(s * step, step)]
        pltpu.make_async_copy(others, others, last_recv.at[s]).wait()

    @pl.loop(0, subsets - 1)
    def _(s):
        pl.when(s == (subsets - 1) // 2)(energy_on)
        arrived(s)
        for k in range(step // 2):
            first = s * step + 2 * k
            y = y_acc[s * (step // 2) + k] + rows_of(m - 1, first)

            def store(i, lines, value):
                image_ref[first + i, lines, :] = value

            second_stage(y, twist_ref, b_hi_ref, b_lo_ref, store)

    for c in range(n):
        if relay and c == RELAY:
            relay_done()
            continue
        sent = stage[c].at[pl.ds(0, rows - piece)]
        pltpu.make_async_copy(sent, sent, part_send.at[c]).wait()
    for u in range(len(units)):
        for i in reach:
            pl.when(p >= i + 1)(lambda u=u, i=i: halo(u, i).wait_send())
    share_wait(e_rng, rng_count, 1)
    mean = jnp.sum(jnp.sum(e_rng[...], axis=0), axis=(0, 1), keepdims=True) / cells
    scale_ref[...] = jnp.broadcast_to(lax.rsqrt(mean + 1e-06), scale_ref.shape)
    arrived(subsets - 1)


def fused(spec, src, offsets, weights, tables, chunks, sets, counts, step, rng_count, az_count):
    rows, columns = spec.shape[:2]
    blocks = rows // BLOCK
    piece = rows // az_count
    m = len(sets)
    units = units_of(chunks)
    total_groups = columns // 2 * az_count
    cells = float(rows * rng_count * total_groups * GW) * float(total_groups * GW)
    hbm = pl.BlockSpec(memory_space=pl.ANY)
    tile = (8, GW)
    dma = pltpu.SemaphoreType.DMA
    vmem = pltpu.VMEM
    f32 = jnp.float32
    sizes = [size for _, size in chunks]
    relay = [vmem((az_count // 2, piece, 1, 1, GW), f32)] if relays(chunks, rng_count, az_count) else []
    outs = [
        vmem(((piece - step), 2 * total_groups, GW), f32),
        vmem((piece // 2, 2 * total_groups, 2 * GW), f32),
        vmem((az_count, piece + PAD, sizes[-1], 1, GW), f32),
        vmem(tile, f32),
    ] + [vmem(t.shape, t.dtype) for t in tables[m - 1:]]
    return pl.pallas_call(
        functools.partial(fused_kernel, rows, blocks, chunks, sets, units, counts, step, cells),
        out_shape=outs,
        in_specs=[hbm] * (4 + len(tables)),
        out_specs=[pl.BlockSpec(memory_space=vmem)] * len(outs),
        scratch_shapes=[vmem((rows + sum(counts) + UNUSED, width, 1, GW), f32) for _, _, width in units]
        + [vmem((rows, size, 1, GW), f32) for size in sizes]
        + [vmem((az_count, piece + PAD, size, 1, GW), f32) for size in sizes[:-1]]
        + [vmem(t.shape, t.dtype) for t in tables[:m - 1]]
        + [
            pltpu.SMEM(src.shape, src.dtype),
            vmem(offsets.shape, offsets.dtype),
            vmem(weights.shape, weights.dtype),
            vmem(tile, f32),
            vmem((az_count,) + tile, f32),
            vmem(tile, f32),
            vmem((rng_count,) + tile, f32),
            dma((3,)),
            dma((len(tables),)),
            dma((len(units),)),
            dma((len(units), len(counts))),
            dma((len(units), len(counts))),
            dma((len(chunks),)),
            dma((len(chunks),)),
            dma((piece // step,)),
            dma((2,)),
            dma((2,)),
            dma((3,)),
        ] + relay,
        compiler_params=pltpu.CompilerParams(
            has_side_effects=True, collective_id=0, vmem_limit_bytes=40 * 1024 * 1024),
    )(src, offsets, weights, spec, *tables)


def store_kernel(step, band_ref, y_acc, recv, scale_ref, a_ref, twist_ref, b_hi_ref, b_lo_ref, out_ref, scaled, sem, end_sem):
    done = band_ref.shape[0]
    scale = scale_ref[:1, :1]

    def copy(first, count, at):
        return pltpu.make_async_copy(scaled.at[pl.ds(first, count)], out_ref.at[pl.ds(first, count)], at)

    @pl.loop(0, done // step)
    def _(i):
        rows = pl.ds(i * step, step)
        scaled[rows] = band_ref[rows] * scale
        copy(i * step, step, sem.at[i]).start()

    for k in range(step // 2):
        first = done + 2 * k
        y = y_acc[first // 2] + first_stage([recv], a_ref, first)

        def store(i, lines, value, first=first):
            scaled[first + i, lines, :] = value * scale

        second_stage(y, twist_ref, b_hi_ref, b_lo_ref, store)
        copy(first, 2, end_sem.at[k]).start()

    @pl.loop(0, done // step)
    def _(i):
        copy(i * step, step, sem.at[i]).wait()

    @pl.loop(0, step // 2)
    def _(k):
        copy(done + 2 * k, 2, end_sem.at[k]).wait()


def store(step, rows, band, *rest):
    parts = rows // step
    vmem = pltpu.VMEM
    shape = (rows,) + band.shape[1:]
    return pl.pallas_call(
        functools.partial(store_kernel, step),
        out_shape=jax.ShapeDtypeStruct(shape, band.dtype),
        in_specs=[pl.BlockSpec(memory_space=vmem)] * (1 + len(rest)),
        out_specs=pl.BlockSpec(memory_space=pl.ANY),
        scratch_shapes=[vmem(shape, band.dtype), pltpu.SemaphoreType.DMA((parts - 1,)),
                        pltpu.SemaphoreType.DMA((step // 2,))],
        compiler_params=pltpu.CompilerParams(vmem_limit_bytes=20 * 1024 * 1024),
    )(band, *rest)


def halo_counts(rows_dev, rng_count):
    total = rows_dev * rng_count
    halo = min(rows_dev - BLOCK + SHIFT_B * BLOCK, total - 2 * BLOCK) + WINDOW - rows_dev
    counts = []
    while halo > 0:
        counts.append(min(halo, rows_dev) if halo > rows_dev else halo - UNUSED)
        halo -= rows_dev
    return counts


def body(spectrum, src_block, offsets, tap_weights):
    rows_dev = spectrum.shape[0]
    columns = spectrum.shape[2]
    groups = columns // GW
    rng_count = lax.axis_size("rng")
    az_count = lax.axis_size("az")
    rows_after = rows_dev // az_count
    total_len = columns * az_count
    chunks = plan(groups)
    sets = gather_sets(chunks, relays(chunks, rng_count, az_count))
    tables = [jnp.asarray(t) for t in dft_tables(az_count, groups, chunks, sets)]
    spec = spectrum.reshape(rows_dev, 2, groups, GW).transpose(0, 2, 1, 3).reshape(rows_dev, 2 * groups, 1, GW)
    counts = halo_counts(rows_dev, rng_count)
    step = min(STEP, rows_after // 2)
    held = fused(spec, src_block.T, offsets, tap_weights, tables, chunks, sets, counts, step, rng_count, az_count)
    image = store(step, rows_after, *held)
    return (
        image.reshape(rows_after, total_len // GW, 2, GW)
        .transpose(0, 2, 1, 3)
        .reshape(rows_after, 2, total_len)
    )


def solution(mesh):
    placed = (P("rng", None, "az"), P("az", "rng"), P("az", "rng"), P(None, "az", "rng"))
    return jax.shard_map(
        body, mesh=mesh, in_specs=placed, out_specs=P(("rng", "az"), None, None), check_vma=False
    )
```
